32 devices in a mesh: dp: 2 (over core), wide: 4 (over y, x), narrow: 4 (over z).
Axes of the slice: x: 2, y: 2, z: 4, core: 2. Of those that a mesh axis runs over, the one named last changes fastest.
Arguments:
- block_input: float32 [1600, 4096], P('wide', ('dp', 'narrow')), as said below
- block_cotangent: float32 [1600, 4096], P('wide', ('dp', 'narrow')), may hold values from -6 to 6
- seq_start: int32 [32, 128], P(('dp', 'wide', 'narrow')), may hold values from 0 to 127, as said below
- ln1_gain: float32 [1600], P('wide'), may hold values from 0.5 to 1.5
- ln1_shift: float32 [1600], P('wide'), may hold values from -2 to 2
- w_qkv: float32 [1600, 3, 1600], P('wide', None, 'narrow'), may hold values from -0.15625 to 0.15625
- b_qv: float32 [2, 1600], P(None, 'narrow'), may hold values from -3 to 3
- w_out: float32 [1600, 1600], P('wide', 'narrow'), may hold values from -0.4375 to 0.4375
- b_out: float32 [1600], P('wide'), may hold values from -2 to 2
- ln2_gain: float32 [1600], P('wide'), may hold values from 0.5 to 1.5
- ln2_shift: float32 [1600], P('wide'), may hold values from -2 to 2
- w_fc: float32 [1600, 6400], P('wide', 'narrow'), may hold values from -0.15625 to 0.15625
- b_fc: float32 [6400], P('narrow'), may hold values from -3 to 3
- w_proj: float32 [1600, 6400], P('wide', 'narrow'), may hold values from -0.078125 to 0.078125
- b_proj: float32 [1600], P('wide'), may hold values from -2 to 2
Outputs:
- block_output: float32 [1600, 4096], P('wide', ('dp', 'narrow'))
- input_grad: float32 [1600, 4096], P('wide', ('dp', 'narrow'))
- grad_ln1_gain: float32 [1600], P('wide')
- grad_ln1_shift: float32 [1600], P('wide')
- grad_w_qkv: float32 [1600, 3, 1600], P('wide', None, 'narrow')
- grad_b_qv: float32 [2, 1600], P(None, 'narrow')
- grad_w_out: float32 [1600, 1600], P('wide', 'narrow')
- grad_b_out: float32 [1600], P('wide')
- grad_ln2_gain: float32 [1600], P('wide')
- grad_ln2_shift: float32 [1600], P('wide')
- grad_w_fc: float32 [1600, 6400], P('wide', 'narrow')
- grad_b_fc: float32 [6400], P('narrow')
- grad_w_proj: float32 [1600, 6400], P('wide', 'narrow')
- grad_b_proj: float32 [1600], P('wide')
The draws below stay inside these ranges and needn't reach their ends.
Inputs may be any that keep to these rules, and one draw needn't show every extreme that they name: `block_input`: token activations of order one, with scales that differ from token to token. `seq_start`: along each row the values never fall; each equals the token's own position at the first token of its sequence and the start of its sequence after it. Block 0 holds one sequence of 128 tokens; some block ends with a sequence of one token.
All inputs are finite; a program needn't handle non-finite values.
Results may differ from the reference program's by a relative error of at most 0.011.
Values may be sent and summed in bfloat16 or wider, within the bound.
A program may use at most 320 MiB of HBM per device.

```python
import math
import jax
import jax.numpy as jnp
from jax import lax

D = 1600
HEADS = 25
HEAD = 64
FF = 6400
TOK_DEV = 128
TOKENS = 4096
BLOCKS = 32


def draw_block_input(key, part):
    value_key, scale_key = jax.random.split(key, 2)
    feature = jnp.arange(D, dtype=jnp.float32) / (D - 1)
    feature_scale = (0.6 * jnp.exp(math.log(3.0) * feature))[:, None]
    token_scale = 0.3 * jnp.exp(jax.random.uniform(scale_key, (1, TOKENS), jnp.float32, 0.0, math.log(10.0)))
    values = jax.random.normal(value_key, (D, TOKENS), jnp.float32) * feature_scale * token_scale
    return values


def draw_seq_start(key, part):
    gap_key, boundary_key = jax.random.split(key)
    block_row = jnp.arange(BLOCKS)[:, None]
    position = jnp.arange(TOK_DEV)[None, :]
    mean_gap = jax.random.randint(gap_key, (BLOCKS, 1), 2, 24) + jnp.where(block_row < BLOCKS // 2, 40, 0)
    boundary = jax.random.randint(boundary_key, (BLOCKS, TOK_DEV), 0, 1 << 20) % mean_gap == 0
    boundary = boundary | (position == 0)
    boundary = jnp.where(block_row == 0, position == 0, boundary)
    boundary = boundary | (block_row == 1) & (position == TOK_DEV - 1)
    starts = lax.cummax(jnp.where(boundary, position, 0), axis=1)
    return starts.astype(jnp.int32)


def block_levels(stream_key, extent, shards, least, largest):
    factor_of, own = 1.0, jax.random.fold_in(stream_key, 6)
    for dim, parts in shards:
        draws = jnp.exp(jax.random.uniform(jax.random.fold_in(own, dim), (parts,), jnp.float32, least / len(shards), largest / len(shards)))
        factor_of = factor_of * jnp.repeat(draws, extent[dim] // parts).reshape([-1 if axis == dim else 1 for axis in range(len(extent))])
    return factor_of


def bell_draw(key, shape, spread, bound, cuts=(), held_as=jnp.bfloat16):
    drawn = spread * jax.random.normal(key, shape, jnp.float32)
    if cuts:
        drawn = drawn * block_levels(key, shape, cuts, -0.22, 0.18)
    return jnp.clip(drawn, -bound, bound).astype(held_as)


def setup_inputs(seed: int = 0) -> dict:
    seeds = jax.random.split(jax.random.key(seed), 16)
    block_input = draw_block_input(jax.random.fold_in(seeds[15], 71), 0)
    block_cotangent = bell_draw(seeds[1], (D, TOKENS), 1.0, 6.0, ((0, 4), (1, 8)), jnp.float32)
    seq_start = draw_seq_start(jax.random.fold_in(seeds[15], 71), 0)
    ln1_gain = jnp.clip(1.0 + 0.1 * jax.random.normal(seeds[3], (D,), jnp.float32), 0.5, 1.5)
    ln1_shift = bell_draw(seeds[4], (D,), 0.3, 2.0, ((0, 4),), jnp.float32)
    w_qkv = bell_draw(seeds[5], (D, 3, D), D ** -0.5, 0.15625, ((0, 4), (2, 4)), jnp.float32)
    b_qv = bell_draw(seeds[6], (2, D), 0.5, 3.0, ((1, 4),), jnp.float32)
    w_out = bell_draw(seeds[7], (D, D), (D // 8) ** -0.5, 0.4375, ((0, 4), (1, 4)), jnp.float32)
    b_out = bell_draw(seeds[8], (D,), 0.3, 2.0, ((0, 4),), jnp.float32)
    ln2_gain = jnp.clip(1.0 + 0.1 * jax.random.normal(seeds[9], (D,), jnp.float32), 0.5, 1.5)
    ln2_shift = bell_draw(seeds[10], (D,), 0.3, 2.0, ((0, 4),), jnp.float32)
    w_fc = bell_draw(seeds[11], (D, FF), D ** -0.5, 0.15625, ((0, 4), (1, 4)), jnp.float32)
    b_fc = bell_draw(seeds[12], (FF,), 0.5, 3.0, ((0, 4),), jnp.float32)
    w_proj = bell_draw(seeds[13], (D, FF), FF ** -0.5, 0.078125, ((0, 4), (1, 4)), jnp.float32)
    b_proj = bell_draw(seeds[14], (D,), 0.3, 2.0, ((0, 4),), jnp.float32)
    return {"block_input": block_input, "block_cotangent": block_cotangent, "seq_start": seq_start, "ln1_gain": ln1_gain, "ln1_shift": ln1_shift, "w_qkv": w_qkv, "b_qv": b_qv, "w_out": w_out, "b_out": b_out, "ln2_gain": ln2_gain, "ln2_shift": ln2_shift, "w_fc": w_fc, "b_fc": b_fc, "w_proj": w_proj, "b_proj": b_proj}


EPS = 1e-05
GELU_C = math.sqrt(2.0 / math.pi)

def rounded(values):
    return lax.optimization_barrier(values.astype(jnp.bfloat16)).astype(jnp.float32)

def gelu_value(pre_act):
    inner = GELU_C * (pre_act + 0.044715 * pre_act * pre_act * pre_act)
    return 0.5 * pre_act * (1.0 + jnp.tanh(inner))

def gelu_slope(pre_act):
    tanh_part = jnp.tanh(GELU_C * (pre_act + 0.044715 * pre_act * pre_act * pre_act))
    return 0.5 * (1.0 + tanh_part) + 0.5 * pre_act * (1.0 - tanh_part * tanh_part) * GELU_C * (1.0 + 3.0 * 0.044715 * pre_act * pre_act)

def norm_forward(inputs, gain, shift):
    mean_row = lax.optimization_barrier(jnp.mean(inputs, axis=-1, keepdims=True))
    variance = lax.optimization_barrier(jnp.mean(inputs * inputs, axis=-1, keepdims=True)) - mean_row * mean_row
    inv_std = lax.rsqrt(variance + EPS)
    normed = (inputs - mean_row) * inv_std
    return (normed, inv_std, (normed * gain + shift).astype(jnp.bfloat16))

def norm_backward(row_grads, normed, inv_std, gain):
    scaled = row_grads * gain
    return inv_std * (scaled - lax.optimization_barrier(jnp.mean(scaled, axis=-1, keepdims=True)) - normed * lax.optimization_barrier(jnp.mean(scaled * normed, axis=-1, keepdims=True)))

def pair_mask(starts):
    position = jnp.arange(starts.shape[-1])
    causal = position[None, :] <= position[:, None]
    same_seq = starts[:, :, None] == starts[:, None, :]
    return (causal[None] & same_seq)[:, None]

def head_split(values, group_count):
    return values.astype(jnp.float32).reshape(group_count, -1, HEADS, HEAD)

def attention_forward(qkv, allowed, group_count):
    score_scale = 1.0 / math.sqrt(HEAD)
    queries = head_split(qkv[:, 0], group_count)
    keys_part = head_split(qkv[:, 1], group_count)
    values_part = head_split(qkv[:, 2], group_count)
    scores = jnp.einsum('bihd,bjhd->bhij', queries, keys_part) * score_scale
    log_total = jnp.log(lax.optimization_barrier(jnp.sum(jnp.where(allowed, jnp.exp(scores), 0.0), axis=-1, keepdims=True)))
    attn_probs = rounded(jnp.where(allowed, jnp.exp(scores - log_total), 0.0))
    attended = jnp.einsum('bhij,bjhd->bihd', attn_probs, values_part)
    return (attended.reshape(-1, HEADS * HEAD).astype(jnp.bfloat16), log_total)

def attention_backward(qkv, allowed, log_total, attended_cot, group_count):
    score_scale = 1.0 / math.sqrt(HEAD)
    queries = head_split(qkv[:, 0], group_count)
    keys_part = head_split(qkv[:, 1], group_count)
    values_part = head_split(qkv[:, 2], group_count)
    scores = jnp.einsum('bihd,bjhd->bhij', queries, keys_part) * score_scale
    probs_full = jnp.where(allowed, jnp.exp(scores - log_total), 0.0)
    cot_heads = head_split(attended_cot, group_count)
    dprobs = jnp.einsum('bihd,bjhd->bhij', cot_heads, values_part)
    row_delta = lax.optimization_barrier(jnp.sum(probs_full * dprobs, axis=-1, keepdims=True))
    score_cot = rounded(probs_full * (dprobs - row_delta) * score_scale)
    query_grad = jnp.einsum('bhij,bjhd->bihd', score_cot, keys_part)
    key_grad = jnp.einsum('bhij,bihd->bjhd', score_cot, queries)
    value_grad = jnp.einsum('bhij,bihd->bjhd', rounded(probs_full), cot_heads)
    stacked = jnp.stack([query_grad, key_grad, value_grad], axis=2)
    return stacked.reshape(-1, 3, HEADS * HEAD)

def reference(block_input, block_cotangent, seq_start, ln1_gain, ln1_shift, w_qkv, b_qv, w_out, b_out, ln2_gain, ln2_shift, w_fc, b_fc, w_proj, b_proj):
    blocks = seq_start.shape[0]
    group_count = math.gcd(blocks, max(1, 4096 // TOK_DEV))
    group_rows = group_count * TOK_DEV
    group_turns = blocks // group_count
    rows_input = block_input.T
    rows_cot = block_cotangent.T
    wq_bf = w_qkv.astype(jnp.bfloat16).reshape(D, 3 * D)
    wo_bf = w_out.T.astype(jnp.bfloat16)
    wf_bf = w_fc.astype(jnp.bfloat16)
    wp_bf = w_proj.T.astype(jnp.bfloat16)
    bias_three = jnp.stack([b_qv[0], jnp.zeros_like(b_qv[0]), b_qv[1]])

    def one_group(running, inputs):
        group_input, group_cot, starts = inputs
        allowed = pair_mask(starts)
        normed_one, inv_one, norm_one = norm_forward(group_input, ln1_gain, ln1_shift)
        qkv = (jnp.dot(norm_one, wq_bf, preferred_element_type=jnp.float32).reshape(group_rows, 3, D) + bias_three).astype(jnp.bfloat16)
        attended, log_total = attention_forward(qkv, allowed, group_count)
        residual = group_input + jnp.dot(attended, wo_bf, preferred_element_type=jnp.float32) + b_out
        normed_two, inv_two, norm_two = norm_forward(residual, ln2_gain, ln2_shift)
        pre_act = jnp.dot(norm_two, wf_bf, preferred_element_type=jnp.float32) + b_fc
        hidden = gelu_value(pre_act).astype(jnp.bfloat16)
        block_output = residual + jnp.dot(hidden, wp_bf, preferred_element_type=jnp.float32) + b_proj
        cot_rows = group_cot.astype(jnp.bfloat16)
        grad_b_proj = lax.optimization_barrier(jnp.sum(group_cot, axis=0))
        grad_w_proj = jnp.dot(hidden.T, cot_rows, preferred_element_type=jnp.float32)
        pre_grad = jnp.dot(cot_rows, wp_bf.T, preferred_element_type=jnp.float32) * gelu_slope(pre_act)
        pre_cot = pre_grad.astype(jnp.bfloat16)
        grad_b_fc = lax.optimization_barrier(jnp.sum(pre_grad, axis=0))
        grad_w_fc = jnp.dot(norm_two.T, pre_cot, preferred_element_type=jnp.float32)
        norm_two_grad = jnp.dot(pre_cot, wf_bf.T, preferred_element_type=jnp.float32)
        grad_ln2_gain = lax.optimization_barrier(jnp.sum(norm_two_grad * normed_two, axis=0))
        grad_ln2_shift = lax.optimization_barrier(jnp.sum(norm_two_grad, axis=0))
        resid_grad = group_cot + norm_backward(norm_two_grad, normed_two, inv_two, ln2_gain)
        resid_cot = resid_grad.astype(jnp.bfloat16)
        grad_b_out = lax.optimization_barrier(jnp.sum(resid_grad, axis=0))
        grad_w_out = jnp.dot(attended.T, resid_cot, preferred_element_type=jnp.float32)
        attended_cot = jnp.dot(resid_cot, wo_bf.T, preferred_element_type=jnp.float32).astype(jnp.bfloat16)
        qkv_grad = attention_backward(qkv, allowed, log_total, attended_cot, group_count)
        grad_b_qv = jnp.stack([lax.optimization_barrier(jnp.sum(qkv_grad[:, 0], axis=0)), lax.optimization_barrier(jnp.sum(qkv_grad[:, 2], axis=0))])
        qkv_cot = qkv_grad.astype(jnp.bfloat16).reshape(group_rows, 3 * D)
        grad_w_qkv = jnp.dot(norm_one.T, qkv_cot, preferred_element_type=jnp.float32).reshape(D, 3, D)
        norm_one_grad = jnp.dot(qkv_cot, wq_bf.T, preferred_element_type=jnp.float32)
        grad_ln1_gain = lax.optimization_barrier(jnp.sum(norm_one_grad * normed_one, axis=0))
        grad_ln1_shift = lax.optimization_barrier(jnp.sum(norm_one_grad, axis=0))
        input_grad = resid_grad + norm_backward(norm_one_grad, normed_one, inv_one, ln1_gain)
        new_grads = (grad_ln1_gain, grad_ln1_shift, grad_w_qkv, grad_b_qv, grad_w_out, grad_b_out, grad_ln2_gain, grad_ln2_shift, grad_w_fc, grad_b_fc, grad_w_proj, grad_b_proj)
        return (jax.tree.map(jnp.add, running, new_grads), (block_output, input_grad))
    initial = (jnp.zeros((D,), jnp.float32), jnp.zeros((D,), jnp.float32), jnp.zeros((D, 3, D), jnp.float32), jnp.zeros((2, D), jnp.float32), jnp.zeros((D, D), jnp.float32), jnp.zeros((D,), jnp.float32), jnp.zeros((D,), jnp.float32), jnp.zeros((D,), jnp.float32), jnp.zeros((D, FF), jnp.float32), jnp.zeros((FF,), jnp.float32), jnp.zeros((FF, D), jnp.float32), jnp.zeros((D,), jnp.float32))
    inputs = (rows_input.reshape(group_turns, group_rows, D), rows_cot.reshape(group_turns, group_rows, D), seq_start.reshape(group_turns, group_count, TOK_DEV))
    running, outputs = lax.scan(one_group, initial, inputs)
    block_output = outputs[0].reshape(-1, D).T
    input_grad = outputs[1].reshape(-1, D).T
    return (block_output, input_grad, running[0], running[1], running[2], running[3], running[4].T, running[5], running[6], running[7], running[8], running[9], running[10].T, running[11])
```

```python
import math

import jax
import jax.numpy as jnp
from jax import lax
from jax.sharding import PartitionSpec as P

HEADS = 25
HEAD = 64

EPS = 1e-05
GELU_C = math.sqrt(2.0 / math.pi)
BF = jnp.bfloat16
F32 = jnp.float32
ZC = ("narrow", "dp")


def gelu_value(pre_act):
    inner = GELU_C * (pre_act + 0.044715 * pre_act * pre_act * pre_act)
    return 0.5 * pre_act * (1.0 + jnp.tanh(inner))


def gelu_slope(pre_act):
    tanh_part = jnp.tanh(GELU_C * (pre_act + 0.044715 * pre_act * pre_act * pre_act))
    return 0.5 * (1.0 + tanh_part) + 0.5 * pre_act * (1.0 - tanh_part * tanh_part) * GELU_C * (
        1.0 + 3.0 * 0.044715 * pre_act * pre_act
    )


def dot(a, b, ca, cb):
    return lax.dot_general(a, b, (((ca,), (cb,)), ((), ())), preferred_element_type=F32)


def row_totals(first_term, second_term):
    return lax.psum(
        (jnp.sum(first_term, axis=1, keepdims=True), jnp.sum(second_term, axis=1, keepdims=True)),
        "wide",
    )


def norm_forward(inputs, gain_shard, shift_shard):
    full_width = inputs.shape[1] * lax.axis_size("wide")
    total_sum, square_sum = row_totals(inputs, inputs * inputs)
    mean_row = total_sum / full_width
    inv_std = lax.rsqrt(square_sum / full_width - mean_row * mean_row + EPS)
    normed = (inputs - mean_row) * inv_std
    return (normed, inv_std, (normed * gain_shard + shift_shard).astype(BF))


def norm_backward(row_grads, normed, inv_std, gain_shard):
    full_width = row_grads.shape[1] * lax.axis_size("wide")
    scaled = row_grads * gain_shard
    first_sum, second_sum = row_totals(scaled, scaled * normed)
    return inv_std * (scaled - first_sum / full_width - normed * (second_sum / full_width))


def gather_features(values):
    return lax.all_gather(values, "wide", axis=1, tiled=True)


def gather_tokens(values):
    return lax.all_gather(values, "wide", axis=0, tiled=True)


def sum_features(partial_value):
    return lax.psum_scatter(partial_value.astype(BF), "wide", scatter_dimension=1, tiled=True).astype(F32)


def sum_tokens(partial_value):
    return lax.psum_scatter(partial_value.astype(BF), "wide", scatter_dimension=0, tiled=True).astype(F32)


def block_mask(starts):
    position = jnp.arange(starts.shape[0])
    return (position[None, :] <= position[:, None]) & (starts[:, None] == starts[None, :])


def split_heads(values):
    return values.reshape(values.shape[0], HEADS, HEAD)


def attend_forward(heads_all, allowed):
    score_scale = 1.0 / math.sqrt(HEAD)
    queries = split_heads(heads_all[:, 0])
    keys_part = split_heads(heads_all[:, 1])
    values_part = split_heads(heads_all[:, 2])
    scores = jnp.einsum("ihd,jhd->hij", queries, keys_part, preferred_element_type=F32) * score_scale
    log_total = jnp.log(jnp.sum(jnp.where(allowed, jnp.exp(scores), 0.0), axis=2, keepdims=True))
    attn_probs = jnp.where(allowed, jnp.exp(scores - log_total), 0.0).astype(BF)
    attended = jnp.einsum("hij,jhd->ihd", attn_probs, values_part, preferred_element_type=F32)
    return (attended.reshape(heads_all.shape[0], HEADS * HEAD).astype(BF), log_total)


def attend_backward(heads_all, allowed, log_total, attended_cot):
    score_scale = 1.0 / math.sqrt(HEAD)
    queries = split_heads(heads_all[:, 0])
    keys_part = split_heads(heads_all[:, 1])
    values_part = split_heads(heads_all[:, 2])
    scores = jnp.einsum("ihd,jhd->hij", queries, keys_part, preferred_element_type=F32) * score_scale
    probs_full = jnp.where(allowed, jnp.exp(scores - log_total), 0.0)
    cot_heads = split_heads(attended_cot)
    dprobs = jnp.einsum("ihd,jhd->hij", cot_heads, values_part, preferred_element_type=F32)
    row_delta = jnp.sum(probs_full * dprobs, axis=2, keepdims=True)
    score_cot = (probs_full * (dprobs - row_delta) * score_scale).astype(BF)
    query_grad = jnp.einsum("hij,jhd->ihd", score_cot, keys_part, preferred_element_type=F32)
    key_grad = jnp.einsum("hij,ihd->jhd", score_cot, queries, preferred_element_type=F32)
    value_grad = jnp.einsum("hij,ihd->jhd", probs_full.astype(BF), cot_heads, preferred_element_type=F32)
    stacked = jnp.stack([query_grad, key_grad, value_grad], axis=1)
    return stacked.reshape(heads_all.shape[0], 3, HEADS * HEAD)


def own_half(values, axis):
    half = values.shape[axis] // lax.axis_size("dp")
    return lax.dynamic_slice_in_dim(values, lax.axis_index("dp") * half, half, axis)


def local(
    block_input,
    block_cotangent,
    seq_start,
    ln1_gain,
    ln1_shift,
    w_qkv,
    b_qv,
    w_out,
    b_out,
    ln2_gain,
    ln2_shift,
    w_fc,
    b_fc,
    w_proj,
    b_proj,
):
    cores, wide, narrow = lax.axis_size("dp"), lax.axis_size("wide"), lax.axis_size("narrow")
    w_index, n_index = lax.axis_index("wide"), lax.axis_index("narrow")
    feats, part = w_qkv.shape[0], w_qkv.shape[2]
    width = feats * wide
    hid = w_fc.shape[1]
    piece = hid // wide
    half = piece // cores

    perm = []
    for w in range(wide):
        for n in range(narrow):
            block = n * wide + w
            perm.append((block, w * narrow + n))
    starts = lax.ppermute(seq_start, ("wide", "narrow"), perm)[0]
    allowed = block_mask(starts)

    wq_mine = own_half(w_qkv.astype(BF).reshape(feats, 3 * part), 0)
    wq_all = lax.all_gather(wq_mine, ZC, axis=0)
    wq_all = wq_all.reshape(narrow, feats, 3, part).transpose(1, 2, 0, 3).reshape(feats, 3 * width)
    wo_mine = own_half(w_out.T.astype(BF), 0)
    wo_all = lax.all_gather(wo_mine, ZC, axis=0, tiled=True)

    def split_units(by_units):
        pieces = by_units.reshape(wide, cores, half, feats)
        mine = lax.dynamic_index_in_dim(pieces, lax.axis_index("dp"), 1, keepdims=False)
        mixed = lax.all_to_all(mine, "wide", split_axis=0, concat_axis=0, tiled=True)
        mixed = mixed.transpose(1, 0, 2).reshape(half, width)
        return lax.all_gather(mixed, ZC, axis=0, tiled=True)

    wf_all = split_units(w_fc.astype(BF).T)
    wp_all = split_units(w_proj.astype(BF).T)
    b_fc_mine = lax.all_gather(
        lax.dynamic_slice_in_dim(b_fc, w_index * piece, piece, 0), "narrow", axis=0, tiled=True
    )

    rows_input = block_input.T
    rows_cot = block_cotangent.T
    normed_one, inv_one, norm_one = norm_forward(rows_input, ln1_gain, ln1_shift)
    bias_q, bias_v = lax.all_gather(b_qv, "narrow", axis=1, tiled=True)
    bias_three = jnp.stack([bias_q, jnp.zeros_like(bias_q), bias_v])
    qkv_rows = sum_tokens(dot(norm_one, wq_all, 1, 0))
    heads_all = (qkv_rows.reshape(-1, 3, width) + bias_three).astype(BF)
    attended, log_total = attend_forward(heads_all, allowed)
    attended_all = gather_tokens(attended)
    residual = rows_input + dot(attended_all, wo_all, 1, 0) + b_out
    normed_two, inv_two, norm_two = norm_forward(residual, ln2_gain, ln2_shift)
    norm_two_all = gather_features(norm_two)
    pre_act = dot(norm_two_all, wf_all, 1, 1) + b_fc_mine
    hidden = gelu_value(pre_act).astype(BF)
    output_rows = residual + sum_features(dot(hidden, wp_all, 1, 0)) + b_proj

    cot_all = gather_features(rows_cot.astype(BF))
    pre_grad = dot(cot_all, wp_all, 1, 1) * gelu_slope(pre_act)
    pre_cot = pre_grad.astype(BF)
    norm_two_grad = sum_features(dot(pre_cot, wf_all, 1, 0))

    def reduce_units(grad_units):
        total = lax.psum_scatter(grad_units.astype(BF), ZC, scatter_dimension=0, tiled=True)
        mixed = lax.all_to_all(
            total.reshape(half, wide, feats), "wide", split_axis=1, concat_axis=0, tiled=True
        )
        mixed = mixed.reshape(wide, half, feats)
        both = lax.all_gather(mixed, "dp", axis=1)
        return both.reshape(hid, feats).T.astype(F32)

    grad_w_proj = reduce_units(dot(hidden, cot_all, 0, 0))
    grad_w_fc = reduce_units(dot(pre_cot, norm_two_all, 0, 0))
    resid_grad = rows_cot + norm_backward(norm_two_grad, normed_two, inv_two, ln2_gain)
    resid_cot = resid_grad.astype(BF)
    attended_cot = sum_tokens(dot(resid_cot, wo_all, 1, 1)).astype(BF)
    qkv_grad = attend_backward(heads_all, allowed, log_total, attended_cot)
    qkv_cot_all = gather_tokens(qkv_grad.astype(BF).reshape(-1, 3 * width))
    norm_one_grad = dot(qkv_cot_all, wq_all, 1, 1)

    wo_grad = dot(attended_all, resid_cot, 0, 0)
    wo_grad = lax.psum_scatter(wo_grad.astype(BF), ZC, scatter_dimension=0, tiled=True)
    grad_w_out = lax.all_gather(wo_grad, "dp", axis=0, tiled=True).T.astype(F32)
    wq_grad = dot(norm_one, qkv_cot_all, 0, 0).astype(BF).reshape(feats, 3, narrow, part)
    wq_grad = wq_grad.transpose(2, 0, 1, 3).reshape(narrow * feats, 3 * part)
    wq_grad = lax.psum_scatter(wq_grad, ZC, scatter_dimension=0, tiled=True)
    grad_w_qkv = lax.all_gather(wq_grad, "dp", axis=0, tiled=True).reshape(feats, 3, part).astype(F32)

    grad_input_rows = resid_grad + norm_backward(norm_one_grad, normed_one, inv_one, ln1_gain)

    qkv_sums = jnp.sum(qkv_grad, axis=0)
    fc_sums = jnp.sum(pre_grad, axis=0).reshape(narrow, 1, piece)
    fc_full = jnp.zeros((narrow, wide, piece), F32)
    fc_full = lax.dynamic_update_slice_in_dim(fc_full, fc_sums, w_index, 1)
    bias_qv_sum, fc_sum = lax.psum(
        (jnp.stack([qkv_sums[0], qkv_sums[2]]), fc_full.reshape(narrow * hid)), ("dp", "wide", "narrow")
    )
    grad_b_qv = lax.dynamic_slice_in_dim(bias_qv_sum, n_index * part, part, 1)
    grad_b_fc = lax.dynamic_slice_in_dim(fc_sum, n_index * hid, hid, 0)
    row_terms = (
        jnp.sum(norm_one_grad * normed_one, axis=0),
        jnp.sum(norm_one_grad, axis=0),
        jnp.sum(resid_grad, axis=0),
        jnp.sum(norm_two_grad * normed_two, axis=0),
        jnp.sum(norm_two_grad, axis=0),
        jnp.sum(rows_cot, axis=0),
    )
    gain_one, shift_one, out_bias, gain_two, shift_two, proj_bias = lax.psum(row_terms, ("dp", "narrow"))
    return (
        output_rows.T,
        grad_input_rows.T,
        gain_one,
        shift_one,
        grad_w_qkv,
        grad_b_qv,
        grad_w_out,
        out_bias,
        gain_two,
        shift_two,
        grad_w_fc,
        grad_b_fc,
        grad_w_proj,
        proj_bias,
    )


def solution(mesh):
    return jax.shard_map(
        local,
        mesh=mesh,
        in_specs=(
            P("wide", ("dp", "narrow")),
            P("wide", ("dp", "narrow")),
            P(("dp", "wide", "narrow"), None),
            P("wide"),
            P("wide"),
            P("wide", None, "narrow"),
            P(None, "narrow"),
            P("wide", "narrow"),
            P("wide"),
            P("wide"),
            P("wide"),
            P("wide", "narrow"),
            P("narrow"),
            P("wide", "narrow"),
            P("wide"),
        ),
        out_specs=(
            P("wide", ("dp", "narrow")),
            P("wide", ("dp", "narrow")),
            P("wide"),
            P("wide"),
            P("wide", None, "narrow"),
            P(None, "narrow"),
            P("wide", "narrow"),
            P("wide"),
            P("wide"),
            P("wide"),
            P("wide", "narrow"),
            P("narrow"),
            P("wide", "narrow"),
            P("wide"),
        ),
        check_vma=False,
    )
```

```python
import math

import jax
import jax.numpy as jnp
from jax import lax
from jax.sharding import PartitionSpec as P

HEADS = 25
HEAD = 64

EPS = 1e-05
GELU_C = math.sqrt(2.0 / math.pi)
BF = jnp.bfloat16
F32 = jnp.float32


def gelu_value(pre_act):
    inner = GELU_C * (pre_act + 0.044715 * pre_act * pre_act * pre_act)
    return 0.5 * pre_act * (1.0 + jnp.tanh(inner))


def gelu_slope(pre_act):
    tanh_part = jnp.tanh(GELU_C * (pre_act + 0.044715 * pre_act * pre_act * pre_act))
    return 0.5 * (1.0 + tanh_part) + 0.5 * pre_act * (1.0 - tanh_part * tanh_part) * GELU_C * (
        1.0 + 3.0 * 0.044715 * pre_act * pre_act
    )


def dot(a, b, ca, cb):
    return lax.dot_general(a, b, (((ca,), (cb,)), ((), ())), preferred_element_type=F32)


def row_totals(first_term, second_term):
    return lax.psum(
        (jnp.sum(first_term, axis=1, keepdims=True), jnp.sum(second_term, axis=1, keepdims=True)),
        "wide",
    )


def norm_forward(inputs, gain_shard, shift_shard):
    full_width = inputs.shape[1] * lax.axis_size("wide")
    total_sum, square_sum = row_totals(inputs, inputs * inputs)
    mean_row = total_sum / full_width
    inv_std = lax.rsqrt(square_sum / full_width - mean_row * mean_row + EPS)
    normed = (inputs - mean_row) * inv_std
    return (normed, inv_std, (normed * gain_shard + shift_shard).astype(BF))


def norm_backward(row_grads, normed, inv_std, gain_shard):
    full_width = row_grads.shape[1] * lax.axis_size("wide")
    scaled = row_grads * gain_shard
    first_sum, second_sum = row_totals(scaled, scaled * normed)
    return inv_std * (scaled - first_sum / full_width - normed * (second_sum / full_width))


def gather_tokens(values):
    return lax.all_gather(values, "wide", axis=0, tiled=True)


def gather_narrow(values):
    return lax.all_gather(values, "narrow", axis=0, tiled=True)


def sum_tokens(partial_value):
    return lax.psum_scatter(partial_value.astype(BF), "wide", scatter_dimension=0, tiled=True).astype(F32)


def sum_narrow(partial_value):
    return lax.psum_scatter(partial_value.astype(BF), "narrow", scatter_dimension=0, tiled=True).astype(F32)


def to_tokens(values):
    return lax.all_to_all(values, "wide", split_axis=0, concat_axis=1, tiled=True)


def to_features(values):
    return lax.all_to_all(values, "wide", split_axis=1, concat_axis=0, tiled=True)


def block_mask(starts):
    position = jnp.arange(starts.shape[0])
    return (position[None, :] <= position[:, None]) & (starts[:, None] == starts[None, :])


def split_heads(values):
    return values.reshape(values.shape[0], HEADS, HEAD)


def attend_forward(heads_all, allowed):
    score_scale = 1.0 / math.sqrt(HEAD)
    queries = split_heads(heads_all[:, 0])
    keys_part = split_heads(heads_all[:, 1])
    values_part = split_heads(heads_all[:, 2])
    scores = jnp.einsum("ihd,jhd->hij", queries, keys_part, preferred_element_type=F32) * score_scale
    log_total = jnp.log(jnp.sum(jnp.where(allowed, jnp.exp(scores), 0.0), axis=2, keepdims=True))
    attn_probs = jnp.where(allowed, jnp.exp(scores - log_total), 0.0).astype(BF)
    attended = jnp.einsum("hij,jhd->ihd", attn_probs, values_part, preferred_element_type=F32)
    return (attended.reshape(heads_all.shape[0], HEADS * HEAD).astype(BF), log_total)


def attend_backward(heads_all, allowed, log_total, attended_cot):
    score_scale = 1.0 / math.sqrt(HEAD)
    queries = split_heads(heads_all[:, 0])
    keys_part = split_heads(heads_all[:, 1])
    values_part = split_heads(heads_all[:, 2])
    scores = jnp.einsum("ihd,jhd->hij", queries, keys_part, preferred_element_type=F32) * score_scale
    probs_full = jnp.where(allowed, jnp.exp(scores - log_total), 0.0)
    cot_heads = split_heads(attended_cot)
    dprobs = jnp.einsum("ihd,jhd->hij", cot_heads, values_part, preferred_element_type=F32)
    row_delta = jnp.sum(probs_full * dprobs, axis=2, keepdims=True)
    score_cot = (probs_full * (dprobs - row_delta) * score_scale).astype(BF)
    query_grad = jnp.einsum("hij,jhd->ihd", score_cot, keys_part, preferred_element_type=F32)
    key_grad = jnp.einsum("hij,ihd->jhd", score_cot, queries, preferred_element_type=F32)
    value_grad = jnp.einsum("hij,ihd->jhd", probs_full.astype(BF), cot_heads, preferred_element_type=F32)
    stacked = jnp.stack([query_grad, key_grad, value_grad], axis=1)
    return stacked.reshape(heads_all.shape[0], 3, HEADS * HEAD)


def own_half(values, axis):
    half = values.shape[axis] // lax.axis_size("dp")
    return lax.dynamic_slice_in_dim(values, lax.axis_index("dp") * half, half, axis)


def local(
    block_input,
    block_cotangent,
    seq_start,
    ln1_gain,
    ln1_shift,
    w_qkv,
    b_qv,
    w_out,
    b_out,
    ln2_gain,
    ln2_shift,
    w_fc,
    b_fc,
    w_proj,
    b_proj,
):
    cores, wide, narrow = lax.axis_size("dp"), lax.axis_size("wide"), lax.axis_size("narrow")
    w_index, n_index = lax.axis_index("wide"), lax.axis_index("narrow")
    feats, part = w_qkv.shape[0], w_qkv.shape[2]
    width = feats * wide
    hid = w_fc.shape[1]

    perm = []
    for w in range(wide):
        for n in range(narrow):
            block = n * wide + w
            perm.append((block, w * narrow + n))
    starts = lax.ppermute(seq_start, ("wide", "narrow"), perm)[0]
    allowed = block_mask(starts)

    wq_mine = own_half(w_qkv.astype(BF).reshape(feats, 3 * part), 0)
    wq_all = lax.all_gather(wq_mine, ("narrow", "dp"), axis=0, tiled=True)
    wq_all = wq_all.reshape(narrow, feats, 3 * part)
    wo_mine = lax.all_gather(own_half(w_out.astype(BF), 0), "narrow", axis=1, tiled=True)
    wo_all = lax.all_gather(wo_mine, ("wide", "dp"), axis=0, tiled=True)
    wf_all = lax.all_gather(own_half(w_fc.astype(BF), 0), ("wide", "dp"), axis=0, tiled=True)
    wp_all = lax.all_gather(own_half(w_proj.astype(BF), 0), ("wide", "dp"), axis=0, tiled=True)
    b_out_full, gain_two_full, shift_two_full = lax.all_gather(
        jnp.stack([b_out, ln2_gain, ln2_shift]), "wide", axis=1, tiled=True
    )
    bias_qv = lax.all_gather(b_qv, "narrow", axis=0).reshape(narrow, 1, 2, part)
    bias_three = jnp.concatenate(
        [bias_qv[:, :, 0], jnp.zeros((narrow, 1, part), F32), bias_qv[:, :, 1]], axis=2
    )

    rows_input = block_input.T
    rows_cot = block_cotangent.T
    x_tok = to_tokens(rows_input)
    dy_tok = to_tokens(rows_cot)
    cot_all = gather_narrow(dy_tok.astype(BF))

    normed_one, inv_one, norm_one = norm_forward(rows_input, ln1_gain, ln1_shift)
    qkv_part = jnp.einsum("tk,nkc->tnc", norm_one, wq_all, preferred_element_type=F32)
    qkv_rows = sum_tokens(qkv_part.transpose(0, 1, 2)).transpose(1, 0, 2)
    qkv_rows = (qkv_rows + bias_three).astype(BF)
    heads_all = qkv_rows.reshape(narrow, -1, 3, part).transpose(1, 2, 0, 3).reshape(-1, 3, width)
    attended, log_total = attend_forward(heads_all, allowed)
    residual = x_tok + dot(attended, wo_all, 1, 1) + b_out_full
    mean_two = jnp.mean(residual, axis=1, keepdims=True)
    inv_two = lax.rsqrt(jnp.mean(residual * residual, axis=1, keepdims=True) - mean_two * mean_two + EPS)
    normed_two = (residual - mean_two) * inv_two
    norm_two = (normed_two * gain_two_full + shift_two_full).astype(BF)
    norm_two_all = gather_narrow(norm_two)
    pre_act = dot(norm_two_all, wf_all, 1, 0) + b_fc
    hidden = gelu_value(pre_act).astype(BF)
    out_tok = residual + sum_narrow(dot(hidden, wp_all, 1, 1))
    output_rows = to_features(out_tok) + b_proj

    pre_grad = dot(cot_all, wp_all, 1, 0) * gelu_slope(pre_act)
    pre_cot = pre_grad.astype(BF)
    norm_two_grad = sum_narrow(dot(pre_cot, wf_all, 1, 1))

    def reduce_wide(grad):
        total = lax.psum_scatter(grad.astype(BF), ("wide", "dp"), scatter_dimension=0, tiled=True)
        return total

    def share(total):
        return lax.all_gather(total, "dp", axis=0, tiled=True).astype(F32)

    grad_w_proj = share(reduce_wide(dot(cot_all, hidden, 0, 0)))
    grad_w_fc = share(reduce_wide(dot(norm_two_all, pre_cot, 0, 0)))

    scaled = norm_two_grad * gain_two_full
    mean_scaled = jnp.mean(scaled, axis=1, keepdims=True)
    mean_cross = jnp.mean(scaled * normed_two, axis=1, keepdims=True)
    resid_grad = dy_tok + inv_two * (scaled - mean_scaled - normed_two * mean_cross)
    resid_cot = resid_grad.astype(BF)
    attended_cot = dot(resid_cot, wo_all, 1, 0).astype(BF)
    wo_grad = reduce_wide(dot(resid_cot, attended, 0, 0))
    wo_grad = lax.psum_scatter(wo_grad, "narrow", scatter_dimension=1, tiled=True)
    grad_w_out = share(wo_grad)

    qkv_grad = attend_backward(heads_all, allowed, log_total, attended_cot)
    qkv_cot = qkv_grad.astype(BF).reshape(-1, 3, narrow, part).transpose(0, 2, 1, 3)
    qkv_cot_all = gather_tokens(qkv_cot.reshape(-1, narrow, 3 * part))
    norm_one_grad = jnp.einsum("tnc,nkc->tk", qkv_cot_all, wq_all, preferred_element_type=F32)
    wq_grad = jnp.einsum("tk,tnc->nkc", norm_one, qkv_cot_all, preferred_element_type=F32).astype(BF)
    wq_grad = lax.psum_scatter(
        wq_grad.reshape(narrow * feats, 3 * part), ("narrow", "dp"), scatter_dimension=0, tiled=True
    )
    grad_w_qkv = share(wq_grad).reshape(feats, 3, part)

    resid_back = to_features(resid_grad)
    grad_input_rows = resid_back + norm_backward(norm_one_grad, normed_one, inv_one, ln1_gain)

    qkv_sums = jnp.sum(qkv_grad, axis=0)
    fc_full = lax.dynamic_update_slice_in_dim(
        jnp.zeros((narrow * hid,), F32), jnp.sum(pre_grad, axis=0), n_index * hid, 0
    )
    token_terms = jnp.stack(
        [
            qkv_sums[0],
            qkv_sums[2],
            jnp.sum(resid_grad, axis=0),
            jnp.sum(norm_two_grad * normed_two, axis=0),
            jnp.sum(norm_two_grad, axis=0),
        ]
    )
    feature_terms = jnp.stack(
        [
            jnp.sum(norm_one_grad * normed_one, axis=0),
            jnp.sum(norm_one_grad, axis=0),
            jnp.sum(rows_cot, axis=0),
        ]
    )
    feature_full = lax.dynamic_update_slice_in_dim(
        jnp.zeros((3, width), F32), feature_terms, w_index * feats, 1
    )
    token_sum, feature_sum, fc_sum = lax.psum((token_terms, feature_full, fc_full), ("dp", "wide", "narrow"))
    grad_b_qv = lax.dynamic_slice_in_dim(token_sum[:2], n_index * part, part, 1)
    out_bias, gain_two, shift_two = lax.dynamic_slice_in_dim(token_sum[2:], w_index * feats, feats, 1)
    gain_one, shift_one, proj_bias = lax.dynamic_slice_in_dim(feature_sum, w_index * feats, feats, 1)
    grad_b_fc = lax.dynamic_slice_in_dim(fc_sum, n_index * hid, hid, 0)
    return (
        output_rows.T,
        grad_input_rows.T,
        gain_one,
        shift_one,
        grad_w_qkv,
        grad_b_qv,
        grad_w_out,
        out_bias,
        gain_two,
        shift_two,
        grad_w_fc,
        grad_b_fc,
        grad_w_proj,
        proj_bias,
    )


def solution(mesh):
    return jax.shard_map(
        local,
        mesh=mesh,
        in_specs=(
            P("wide", ("dp", "narrow")),
            P("wide", ("dp", "narrow")),
            P(("dp", "wide", "narrow"), None),
            P("wide"),
            P("wide"),
            P("wide", None, "narrow"),
            P(None, "narrow"),
            P("wide", "narrow"),
            P("wide"),
            P("wide"),
            P("wide"),
            P("wide", "narrow"),
            P("narrow"),
            P("wide", "narrow"),
            P("wide"),
        ),
        out_specs=(
            P("wide", ("dp", "narrow")),
            P("wide", ("dp", "narrow")),
            P("wide"),
            P("wide"),
            P("wide", None, "narrow"),
            P(None, "narrow"),
            P("wide", "narrow"),
            P("wide"),
            P("wide"),
            P("wide"),
            P("wide", "narrow"),
            P("narrow"),
            P("wide", "narrow"),
            P("wide"),
        ),
        check_vma=False,
    )
```

```python
import math

import jax
import jax.numpy as jnp
from jax import lax
from jax.experimental import pallas as pl
from jax.experimental.pallas import tpu as pltpu
from jax.sharding import PartitionSpec as P

HEADS = 25
HEAD = 64

EPS = 1e-05
GELU_C = math.sqrt(2.0 / math.pi)
BF = jnp.bfloat16
F32 = jnp.float32


def gelu_value(pre_act):
    inner = GELU_C * (pre_act + 0.044715 * pre_act * pre_act * pre_act)
    return 0.5 * pre_act * (1.0 + jnp.tanh(inner))


def gelu_slope(pre_act):
    tanh_part = jnp.tanh(GELU_C * (pre_act + 0.044715 * pre_act * pre_act * pre_act))
    return 0.5 * (1.0 + tanh_part) + 0.5 * pre_act * (1.0 - tanh_part * tanh_part) * GELU_C * (
        1.0 + 3.0 * 0.044715 * pre_act * pre_act
    )


def dot(a, b, ca, cb):
    return lax.dot_general(a, b, (((ca,), (cb,)), ((), ())), preferred_element_type=F32)


def row_totals(first_term, second_term):
    return lax.psum(
        (jnp.sum(first_term, axis=1, keepdims=True), jnp.sum(second_term, axis=1, keepdims=True)),
        "wide",
    )


def norm_forward(inputs, gain_shard, shift_shard):
    full_width = inputs.shape[1] * lax.axis_size("wide")
    total_sum, square_sum = row_totals(inputs, inputs * inputs)
    mean_row = total_sum / full_width
    inv_std = lax.rsqrt(square_sum / full_width - mean_row * mean_row + EPS)
    normed = (inputs - mean_row) * inv_std
    return (normed, inv_std, (normed * gain_shard + shift_shard).astype(BF))


def norm_backward(row_grads, normed, inv_std, gain_shard):
    full_width = row_grads.shape[1] * lax.axis_size("wide")
    scaled = row_grads * gain_shard
    first_sum, second_sum = row_totals(scaled, scaled * normed)
    return inv_std * (scaled - first_sum / full_width - normed * (second_sum / full_width))


def gather_tokens(values):
    return lax.all_gather(values, "wide", axis=0, tiled=True)


def gather_narrow(values):
    return lax.all_gather(values, "narrow", axis=0, tiled=True)


def sum_tokens(partial_value):
    return lax.psum_scatter(partial_value.astype(BF), "wide", scatter_dimension=0, tiled=True).astype(F32)


def sum_narrow(partial_value):
    return lax.psum_scatter(partial_value.astype(BF), "narrow", scatter_dimension=0, tiled=True).astype(F32)


def to_tokens(values):
    return lax.all_to_all(values, "wide", split_axis=0, concat_axis=1, tiled=True)


def to_features(values):
    return lax.all_to_all(values, "wide", split_axis=1, concat_axis=0, tiled=True)


def block_mask(starts):
    position = jnp.arange(starts.shape[0])
    return (position[None, :] <= position[:, None]) & (starts[:, None] == starts[None, :])


def split_heads(values):
    return values.reshape(values.shape[0], HEADS, HEAD)


def attend_forward(heads_all, allowed):
    score_scale = 1.0 / math.sqrt(HEAD)
    queries = split_heads(heads_all[:, 0])
    keys_part = split_heads(heads_all[:, 1])
    values_part = split_heads(heads_all[:, 2])
    scores = jnp.einsum("ihd,jhd->hij", queries, keys_part, preferred_element_type=F32) * score_scale
    log_total = jnp.log(jnp.sum(jnp.where(allowed, jnp.exp(scores), 0.0), axis=2, keepdims=True))
    attn_probs = jnp.where(allowed, jnp.exp(scores - log_total), 0.0).astype(BF)
    attended = jnp.einsum("hij,jhd->ihd", attn_probs, values_part, preferred_element_type=F32)
    return (attended.reshape(heads_all.shape[0], HEADS * HEAD).astype(BF), log_total)


def attend_backward(heads_all, allowed, log_total, attended_cot):
    score_scale = 1.0 / math.sqrt(HEAD)
    queries = split_heads(heads_all[:, 0])
    keys_part = split_heads(heads_all[:, 1])
    values_part = split_heads(heads_all[:, 2])
    scores = jnp.einsum("ihd,jhd->hij", queries, keys_part, preferred_element_type=F32) * score_scale
    probs_full = jnp.where(allowed, jnp.exp(scores - log_total), 0.0)
    cot_heads = split_heads(attended_cot)
    dprobs = jnp.einsum("ihd,jhd->hij", cot_heads, values_part, preferred_element_type=F32)
    row_delta = jnp.sum(probs_full * dprobs, axis=2, keepdims=True)
    score_cot = (probs_full * (dprobs - row_delta) * score_scale).astype(BF)
    query_grad = jnp.einsum("hij,jhd->ihd", score_cot, keys_part, preferred_element_type=F32)
    key_grad = jnp.einsum("hij,ihd->jhd", score_cot, queries, preferred_element_type=F32)
    value_grad = jnp.einsum("hij,ihd->jhd", probs_full.astype(BF), cot_heads, preferred_element_type=F32)
    stacked = jnp.stack([query_grad, key_grad, value_grad], axis=1)
    return stacked.reshape(heads_all.shape[0], 3, HEADS * HEAD)


MESH = pl.DeviceIdType.MESH
VMEM_LIMIT = 60 * 1024 * 1024


def params(collective_id):
    return pltpu.CompilerParams(
        collective_id=collective_id, has_side_effects=True, vmem_limit_bytes=VMEM_LIMIT
    )


def in_vmem(count):
    return [pl.BlockSpec(memory_space=pltpu.VMEM)] * count


def shape_of(shape, dtype):
    return jax.ShapeDtypeStruct(shape, dtype)


def square_peers():
    me = lax.axis_index("wide")
    return me, me + 1 - 2 * lax.rem(me, 2), lax.rem(me + 2, 4), 3 - me


def greet(axis, peers):
    barrier = pltpu.get_barrier_semaphore()
    for peer in peers:
        pl.semaphore_signal(barrier, inc=1, device_id={axis: peer}, device_id_type=MESH)
    pl.semaphore_wait(barrier, len(peers))


def remote(src, dst, send_sem, recv_sem, axis, peer):
    return pltpu.make_async_remote_copy(
        src_ref=src,
        dst_ref=dst,
        send_sem=send_sem,
        recv_sem=recv_sem,
        device_id={axis: peer},
        device_id_type=MESH,
    )


def start_kernel(
    x_ref, dy_ref, gain_ref, shift_ref, vec_ref,
    norm_ref, stat_ref, xt_ref, dyt_ref, vecs_ref,
    sums, all_sums, send_sem, recv_sem, local_sem,
):
    feats, tokens = x_ref.shape
    wide = 4
    block = tokens // wide
    me, xp, yp, dg = square_peers()
    peers = (xp, yp, dg)
    greet("wide", peers)
    x = x_ref[...]
    sums[...] = jnp.zeros_like(sums)
    stat_ref[...] = jnp.zeros_like(stat_ref)
    sums[0:1, :] = jnp.sum(x, axis=0, keepdims=True)
    sums[1:2, :] = jnp.sum(x * x, axis=0, keepdims=True)
    copies = []

    def send(k, j, src, dst, peer):
        copy = remote(src, dst, send_sem.at[k, j], recv_sem.at[k, j], "wide", peer)
        copy.start()
        copies.append(copy)

    mine = pl.ds(me * feats, feats)
    for j, peer in enumerate(peers):
        send(0, j, sums, all_sums.at[me], peer)
    for j, peer in enumerate(peers):
        send(1, j, vec_ref, vecs_ref.at[me], peer)
        theirs = pl.ds(pl.multiple_of(peer * block, 128), block)
        send(2, j, x_ref.at[:, theirs], xt_ref.at[mine, :], peer)
        send(3, j, dy_ref.at[:, theirs], dyt_ref.at[mine, :], peer)
    own = pl.ds(pl.multiple_of(me * block, 128), block)
    xt_ref[mine, :] = x_ref[:, own]
    dyt_ref[mine, :] = dy_ref[:, own]
    vecs_ref[me] = vec_ref[...]
    for j in range(3):
        copies[j].wait()
    total = sums[...]
    for peer in peers:
        total = total + all_sums[peer]
    width = feats * wide
    mean = total[0:1, :] / width
    inv = lax.rsqrt(total[1:2, :] / width - mean * mean + EPS)
    stat_ref[0:1, :] = mean
    stat_ref[1:2, :] = inv
    norm_ref[...] = ((x - mean) * inv * gain_ref[...] + shift_ref[...]).astype(BF)
    for copy in copies[3:]:
        copy.wait()


def start_stage(x, dy, gain, shift, vec):
    feats, tokens = x.shape
    return pl.pallas_call(
        start_kernel,
        out_shape=(
            shape_of((feats, tokens), BF),
            shape_of((8, tokens), F32),
            shape_of((4 * feats, tokens // 4), F32),
            shape_of((4 * feats, tokens // 4), F32),
            shape_of((4,) + vec.shape, F32),
        ),
        in_specs=in_vmem(5),
        out_specs=tuple(in_vmem(5)),
        scratch_shapes=[
            pltpu.VMEM((8, tokens), F32),
            pltpu.VMEM((4, 8, tokens), F32),
            pltpu.SemaphoreType.DMA((4, 3)),
            pltpu.SemaphoreType.DMA((4, 3)),
            pltpu.SemaphoreType.DMA,
        ],
        compiler_params=params(1),
        cost_estimate=pl.CostEstimate(flops=10**9, bytes_accessed=30 * 10**6, transcendentals=0),
        name="start_stage",
    )(x, dy, gain, shift, vec)


def qkv_kernel(
    norm_ref, w_ref, bias_ref, out_ref, acc, first_out, first_in, second_out, second_in, send_sem, recv_sem
):
    pieces, feats, cols = w_ref.shape
    tokens = norm_ref.shape[1]
    block = tokens // 4
    me, xp, yp, dg = square_peers()
    greet("wide", (xp, yp))

    def rows(index):
        return pl.ds(pl.multiple_of(index * block, block), block)

    def ways(p):
        turn = lax.rem(p, 2)
        return xp * (1 - turn) + yp * turn, yp * (1 - turn) + xp * turn

    def first_copy(p):
        return remote(first_out.at[p], first_in.at[p], send_sem.at[0, p], recv_sem.at[0, p], "wide", ways(p)[0])

    def second_copy(p):
        return remote(second_out.at[p], second_in.at[p], send_sem.at[1, p], recv_sem.at[1, p], "wide", ways(p)[1])

    def issue(p, carry):
        acc[p] = dot(norm_ref[...], w_ref[p], 0, 0)
        first_out[p, 0] = acc[p, rows(ways(p)[0]), :].astype(BF)
        first_out[p, 1] = acc[p, rows(dg), :].astype(BF)
        first_copy(p).start()
        return carry

    lax.fori_loop(0, pieces, issue, 0)

    def middle(p, carry):
        first_copy(p).wait()
        second_out[p] = (acc[p, rows(ways(p)[1]), :] + first_in[p, 1].astype(F32)).astype(BF)
        second_copy(p).start()
        return carry

    lax.fori_loop(0, pieces, middle, 0)

    def last(p, carry):
        second_copy(p).wait()
        total = acc[p, rows(me), :] + first_in[p, 0].astype(F32) + second_in[p].astype(F32)
        out_ref[p] = (total + bias_ref[p]).astype(BF)
        return carry

    lax.fori_loop(0, pieces, last, 0)


def qkv_stage(norm, w, bias):
    pieces, feats, cols = w.shape
    tokens = norm.shape[1]
    block = tokens // 4
    return pl.pallas_call(
        qkv_kernel,
        out_shape=shape_of((pieces, block, cols), BF),
        in_specs=in_vmem(3),
        out_specs=pl.BlockSpec(memory_space=pltpu.VMEM),
        scratch_shapes=[
            pltpu.VMEM((pieces, tokens, cols), F32),
            pltpu.VMEM((pieces, 2, block, cols), BF),
            pltpu.VMEM((pieces, 2, block, cols), BF),
            pltpu.VMEM((pieces, block, cols), BF),
            pltpu.VMEM((pieces, block, cols), BF),
            pltpu.SemaphoreType.DMA((2, pieces)),
            pltpu.SemaphoreType.DMA((2, pieces)),
        ],
        compiler_params=params(2),
        cost_estimate=pl.CostEstimate(flops=3 * 10**10, bytes_accessed=10**8, transcendentals=0),
        name="qkv_stage",
    )(norm, w, bias)


def spread_kernel(own_ref, all_ref, send_sem, recv_sem):
    pieces, block, cols = own_ref.shape
    me, xp, yp, dg = square_peers()
    greet("wide", (xp, yp))

    def rows(index):
        return pl.ds(pl.multiple_of(index * block, block), block)

    def ways(p):
        turn = lax.rem(p, 2)
        return xp * (1 - turn) + yp * turn, yp * (1 - turn) + xp * turn

    def own_copy(p, k):
        return remote(
            own_ref.at[p], all_ref.at[p, rows(me), :], send_sem.at[k, p], recv_sem.at[k, p], "wide", ways(p)[k]
        )

    def pass_copy(p):
        source = all_ref.at[p, rows(ways(p)[0]), :]
        return remote(source, source, send_sem.at[2, p], recv_sem.at[2, p], "wide", ways(p)[1])

    def issue(p, carry):
        own_copy(p, 0).start()
        return carry

    def issue_second(p, carry):
        own_copy(p, 1).start()
        all_ref[p, rows(me), :] = own_ref[p]
        return carry

    def relay(p, carry):
        own_copy(p, 0).wait()
        pass_copy(p).start()
        return carry

    def finish(p, carry):
        own_copy(p, 1).wait()
        pass_copy(p).wait()
        return carry

    for step in (issue, issue_second, relay, finish):
        lax.fori_loop(0, pieces, step, 0)


def spread_stage(own):
    pieces, block, cols = own.shape
    return pl.pallas_call(
        spread_kernel,
        out_shape=shape_of((pieces, 4 * block, cols), BF),
        in_specs=in_vmem(1),
        out_specs=pl.BlockSpec(memory_space=pltpu.VMEM),
        scratch_shapes=[pltpu.SemaphoreType.DMA((3, pieces)), pltpu.SemaphoreType.DMA((3, pieces))],
        compiler_params=params(3),
        cost_estimate=pl.CostEstimate(flops=3 * 10**10, bytes_accessed=10**8, transcendentals=0),
        name="spread_stage",
    )(own)


def line_sides():
    n, count = lax.axis_index("narrow"), lax.axis_size("narrow")
    return n, count, n > 0, n < count - 1


def greet_line(n, has_down, has_up):
    barrier = pltpu.get_barrier_semaphore()
    for has, peer in ((has_down, n - 1), (has_up, n + 1)):

        @pl.when(has)
        def _():
            pl.semaphore_signal(barrier, inc=1, device_id={"narrow": peer}, device_id_type=MESH)

    pl.semaphore_wait(barrier, has_down.astype(jnp.int32) + has_up.astype(jnp.int32))


def line_gather_kernel(own_ref, all_ref, send_sem, recv_sem):
    n, count, has_down, has_up = line_sides()
    greet_line(n, has_down, has_up)

    def copy(block, way, src=None):
        place = all_ref.at[block]
        return remote(
            place if src is None else src, place, send_sem.at[way, block], recv_sem.at[block], "narrow", n + 1 - 2 * way
        )

    @pl.when(has_up)
    def _():
        copy(n, 0, own_ref).start()

    @pl.when(has_down)
    def _():
        copy(n, 1, own_ref).start()

    all_ref[n] = own_ref[...]
    for step in range(1, count):
        below, above = n - step, n + step

        @pl.when(below >= 0)
        def _():
            copy(below, 0).wait_recv()

            @pl.when(has_up)
            def _():
                copy(below, 0).start()

        @pl.when(above < count)
        def _():
            copy(above, 1).wait_recv()

            @pl.when(has_down)
            def _():
                copy(above, 1).start()

    for step in range(count):
        below, above = n - step, n + step

        @pl.when((below >= 0) & has_up)
        def _():
            copy(below, 0).wait_send()

        @pl.when((above < count) & has_down)
        def _():
            copy(above, 1).wait_send()


def line_gather(own):
    count = lax.axis_size("narrow")
    return pl.pallas_call(
        line_gather_kernel,
        out_shape=shape_of((count,) + own.shape, own.dtype),
        in_specs=in_vmem(1),
        out_specs=pl.BlockSpec(memory_space=pltpu.VMEM),
        scratch_shapes=[pltpu.SemaphoreType.DMA((2, count)), pltpu.SemaphoreType.DMA((count,))],
        compiler_params=params(4),
        cost_estimate=pl.CostEstimate(flops=2 * 10**10, bytes_accessed=7 * 10**7, transcendentals=0),
        name="line_gather",
    )(own)


def line_sum_kernel(part_ref, out_ref, leave, arrive, send_sem, recv_sem):
    n, count, has_down, has_up = line_sides()
    greet_line(n, has_down, has_up)

    def copy(way, block):
        return remote(
            leave.at[way, block],
            arrive.at[way, block],
            send_sem.at[way, block],
            recv_sem.at[way, block],
            "narrow",
            n + 1 - 2 * way,
        )

    def turn(way, block, sends, joins):
        @pl.when(sends & joins)
        def _():
            copy(way, block).wait_recv()
            leave[way, block] = (part_ref[block].astype(F32) + arrive[way, block].astype(F32)).astype(BF)
            copy(way, block).start()

        @pl.when(sends & jnp.logical_not(joins))
        def _():
            leave[way, block] = part_ref[block]
            copy(way, block).start()

    for step in range(count - 1):
        turn(0, count - 1 - step, n < count - 1 - step, has_down)
        turn(1, step, n > step, has_up)
    out_ref[...] = part_ref[n].astype(F32)

    @pl.when(has_down)
    def _():
        copy(0, n).wait_recv()
        out_ref[...] += arrive[0, n].astype(F32)

    @pl.when(has_up)
    def _():
        copy(1, n).wait_recv()
        out_ref[...] += arrive[1, n].astype(F32)

    for step in range(count - 1):

        @pl.when(n < count - 1 - step)
        def _():
            copy(0, count - 1 - step).wait_send()

        @pl.when(n > step)
        def _():
            copy(1, step).wait_send()


def line_sum(part):
    count, block, cols = part.shape
    return pl.pallas_call(
        line_sum_kernel,
        out_shape=shape_of((block, cols), F32),
        in_specs=in_vmem(1),
        out_specs=pl.BlockSpec(memory_space=pltpu.VMEM),
        scratch_shapes=[
            pltpu.VMEM((2, count, block, cols), BF),
            pltpu.VMEM((2, count, block, cols), BF),
            pltpu.SemaphoreType.DMA((2, count)),
            pltpu.SemaphoreType.DMA((2, count)),
        ],
        compiler_params=params(5),
        cost_estimate=pl.CostEstimate(flops=2 * 10**10, bytes_accessed=7 * 10**7, transcendentals=0),
        name="line_sum",
    )(part)


def own_half(values, axis):
    half = values.shape[axis] // lax.axis_size("dp")
    return lax.dynamic_slice_in_dim(values, lax.axis_index("dp") * half, half, axis)


def local(
    block_input,
    block_cotangent,
    seq_start,
    ln1_gain,
    ln1_shift,
    w_qkv,
    b_qv,
    w_out,
    b_out,
    ln2_gain,
    ln2_shift,
    w_fc,
    b_fc,
    w_proj,
    b_proj,
):
    cores, wide, narrow = lax.axis_size("dp"), lax.axis_size("wide"), lax.axis_size("narrow")
    w_index, n_index = lax.axis_index("wide"), lax.axis_index("narrow")
    feats, part = w_qkv.shape[0], w_qkv.shape[2]
    width = feats * wide
    hid = w_fc.shape[1]

    perm = []
    for w in range(wide):
        for n in range(narrow):
            block = n * wide + w
            perm.append((block, w * narrow + n))
    starts = lax.ppermute(seq_start, ("wide", "narrow"), perm)[0]
    allowed = block_mask(starts)

    wq_mine = own_half(w_qkv.astype(BF).reshape(feats, 3 * part), 0)
    wq_all = lax.all_gather(wq_mine, ("narrow", "dp"), axis=0, tiled=True)
    wq_all = wq_all.reshape(narrow, feats, 3 * part)
    wo_mine = lax.all_gather(own_half(w_out.astype(BF), 0), "narrow", axis=1, tiled=True)
    wo_all = lax.all_gather(wo_mine, ("wide", "dp"), axis=0, tiled=True)
    wf_all = lax.all_gather(own_half(w_fc.astype(BF), 0), ("wide", "dp"), axis=0, tiled=True)
    wp_all = lax.all_gather(own_half(w_proj.astype(BF), 0), ("wide", "dp"), axis=0, tiled=True)
    bias_qv = lax.all_gather(b_qv, "narrow", axis=0).reshape(narrow, 1, 2, part)
    bias_three = jnp.concatenate(
        [bias_qv[:, :, 0], jnp.zeros((narrow, 1, part), F32), bias_qv[:, :, 1]], axis=2
    )

    rows_input = block_input.T
    rows_cot = block_cotangent.T
    square = wide == 4
    if square:
        vec = jnp.zeros((8, feats), F32)
        vec = vec.at[0].set(b_out).at[1].set(ln2_gain).at[2].set(ln2_shift)
        norm_t, stats, x_tok, dy_tok, vecs = start_stage(
            block_input, block_cotangent, ln1_gain[:, None], ln1_shift[:, None], vec
        )
        x_tok, dy_tok = x_tok.T, dy_tok.T
        b_out_full, gain_two_full, shift_two_full = (vecs[:, i].reshape(width) for i in range(3))
        norm_one = norm_t.T
        inv_one = stats[1][:, None]
        normed_one = (rows_input - stats[0][:, None]) * inv_one
        qkv_rows = qkv_stage(norm_t, wq_all, bias_three)
    else:
        b_out_full, gain_two_full, shift_two_full = lax.all_gather(
            jnp.stack([b_out, ln2_gain, ln2_shift]), "wide", axis=1, tiled=True
        )
        x_tok = to_tokens(rows_input)
        dy_tok = to_tokens(rows_cot)
        normed_one, inv_one, norm_one = norm_forward(rows_input, ln1_gain, ln1_shift)
        qkv_part = jnp.einsum("tk,nkc->tnc", norm_one, wq_all, preferred_element_type=F32)
        qkv_rows = sum_tokens(qkv_part).transpose(1, 0, 2)
        qkv_rows = (qkv_rows + bias_three).astype(BF)
    cot_all = gather_narrow(dy_tok.astype(BF))
    heads_all = qkv_rows.reshape(narrow, -1, 3, part).transpose(1, 2, 0, 3).reshape(-1, 3, width)
    attended, log_total = attend_forward(heads_all, allowed)
    residual = x_tok + dot(attended, wo_all, 1, 1) + b_out_full
    mean_two = jnp.mean(residual, axis=1, keepdims=True)
    inv_two = lax.rsqrt(jnp.mean(residual * residual, axis=1, keepdims=True) - mean_two * mean_two + EPS)
    normed_two = (residual - mean_two) * inv_two
    norm_two = (normed_two * gain_two_full + shift_two_full).astype(BF)
    norm_two_all = line_gather(norm_two).reshape(-1, width)
    pre_act = dot(norm_two_all, wf_all, 1, 0) + b_fc
    hidden = gelu_value(pre_act).astype(BF)
    out_tok = residual + sum_narrow(dot(hidden, wp_all, 1, 1))
    output_rows = to_features(out_tok) + b_proj

    pre_grad = dot(cot_all, wp_all, 1, 0) * gelu_slope(pre_act)
    pre_cot = pre_grad.astype(BF)
    norm_two_grad = line_sum(dot(pre_cot, wf_all, 1, 1).astype(BF).reshape(narrow, -1, width))

    def reduce_wide(grad):
        total = lax.psum_scatter(grad.astype(BF), ("wide", "dp"), scatter_dimension=0, tiled=True)
        return total

    def share(total):
        return lax.all_gather(total, "dp", axis=0, tiled=True).astype(F32)

    grad_w_proj = share(reduce_wide(dot(cot_all, hidden, 0, 0)))
    grad_w_fc = share(reduce_wide(dot(norm_two_all, pre_cot, 0, 0)))

    scaled = norm_two_grad * gain_two_full
    mean_scaled = jnp.mean(scaled, axis=1, keepdims=True)
    mean_cross = jnp.mean(scaled * normed_two, axis=1, keepdims=True)
    resid_grad = dy_tok + inv_two * (scaled - mean_scaled - normed_two * mean_cross)
    resid_cot = resid_grad.astype(BF)
    attended_cot = dot(resid_cot, wo_all, 1, 0).astype(BF)
    wo_grad = reduce_wide(dot(resid_cot, attended, 0, 0))
    wo_grad = lax.psum_scatter(wo_grad, "narrow", scatter_dimension=1, tiled=True)
    grad_w_out = share(wo_grad)

    qkv_grad = attend_backward(heads_all, allowed, log_total, attended_cot)
    qkv_cot = qkv_grad.astype(BF).reshape(-1, 3, narrow, part).transpose(2, 0, 1, 3)
    qkv_cot = qkv_cot.reshape(narrow, -1, 3 * part)
    if square:
        qkv_cot_all = spread_stage(qkv_cot)
    else:
        qkv_cot_all = lax.all_gather(qkv_cot, "wide", axis=1, tiled=True)
    norm_one_grad = jnp.einsum("ntc,nkc->tk", qkv_cot_all, wq_all, preferred_element_type=F32)
    wq_grad = jnp.einsum("tk,ntc->nkc", norm_one, qkv_cot_all, preferred_element_type=F32).astype(BF)
    wq_grad = lax.psum_scatter(
        wq_grad.reshape(narrow * feats, 3 * part), ("narrow", "dp"), scatter_dimension=0, tiled=True
    )
    grad_w_qkv = share(wq_grad).reshape(feats, 3, part)

    resid_back = to_features(resid_grad)
    grad_input_rows = resid_back + norm_backward(norm_one_grad, normed_one, inv_one, ln1_gain)

    qkv_sums = jnp.sum(qkv_grad, axis=0)
    fc_full = lax.dynamic_update_slice_in_dim(
        jnp.zeros((narrow * hid,), F32), jnp.sum(pre_grad, axis=0), n_index * hid, 0
    )
    token_terms = jnp.stack(
        [
            qkv_sums[0],
            qkv_sums[2],
            jnp.sum(resid_grad, axis=0),
            jnp.sum(norm_two_grad * normed_two, axis=0),
            jnp.sum(norm_two_grad, axis=0),
        ]
    )
    feature_terms = jnp.stack(
        [
            jnp.sum(norm_one_grad * normed_one, axis=0),
            jnp.sum(norm_one_grad, axis=0),
            jnp.sum(rows_cot, axis=0),
        ]
    )
    feature_full = lax.dynamic_update_slice_in_dim(
        jnp.zeros((3, width), F32), feature_terms, w_index * feats, 1
    )
    token_sum, feature_sum, fc_sum = lax.psum((token_terms, feature_full, fc_full), ("dp", "wide", "narrow"))
    grad_b_qv = lax.dynamic_slice_in_dim(token_sum[:2], n_index * part, part, 1)
    out_bias, gain_two, shift_two = lax.dynamic_slice_in_dim(token_sum[2:], w_index * feats, feats, 1)
    gain_one, shift_one, proj_bias = lax.dynamic_slice_in_dim(feature_sum, w_index * feats, feats, 1)
    grad_b_fc = lax.dynamic_slice_in_dim(fc_sum, n_index * hid, hid, 0)
    return (
        output_rows.T,
        grad_input_rows.T,
        gain_one,
        shift_one,
        grad_w_qkv,
        grad_b_qv,
        grad_w_out,
        out_bias,
        gain_two,
        shift_two,
        grad_w_fc,
        grad_b_fc,
        grad_w_proj,
        proj_bias,
    )


def solution(mesh):
    return jax.shard_map(
        local,
        mesh=mesh,
        in_specs=(
            P("wide", ("dp", "narrow")),
            P("wide", ("dp", "narrow")),
            P(("dp", "wide", "narrow"), None),
            P("wide"),
            P("wide"),
            P("wide", None, "narrow"),
            P(None, "narrow"),
            P("wide", "narrow"),
            P("wide"),
            P("wide"),
            P("wide"),
            P("wide", "narrow"),
            P("narrow"),
            P("wide", "narrow"),
            P("wide"),
        ),
        out_specs=(
            P("wide", ("dp", "narrow")),
            P("wide", ("dp", "narrow")),
            P("wide"),
            P("wide"),
            P("wide", None, "narrow"),
            P(None, "narrow"),
            P("wide", "narrow"),
            P("wide"),
            P("wide"),
            P("wide"),
            P("wide", "narrow"),
            P("narrow"),
            P("wide", "narrow"),
            P("wide"),
        ),
        check_vma=False,
    )
```

```python
import functools
import math

import jax
import jax.numpy as jnp
from jax import lax
from jax.experimental import pallas as pl
from jax.experimental.pallas import tpu as pltpu
from jax.sharding import PartitionSpec as P

HEADS = 25
HEAD = 64

EPS = 1e-05
GELU_C = math.sqrt(2.0 / math.pi)
BF = jnp.bfloat16
F32 = jnp.float32


def gelu_value(pre_act):
    inner = GELU_C * (pre_act + 0.044715 * pre_act * pre_act * pre_act)
    return 0.5 * pre_act * (1.0 + jnp.tanh(inner))


def gelu_slope(pre_act):
    tanh_part = jnp.tanh(GELU_C * (pre_act + 0.044715 * pre_act * pre_act * pre_act))
    return 0.5 * (1.0 + tanh_part) + 0.5 * pre_act * (1.0 - tanh_part * tanh_part) * GELU_C * (
        1.0 + 3.0 * 0.044715 * pre_act * pre_act
    )


def dot(a, b, ca, cb):
    return lax.dot_general(a, b, (((ca,), (cb,)), ((), ())), preferred_element_type=F32)


def row_totals(first_term, second_term):
    return lax.psum(
        (jnp.sum(first_term, axis=1, keepdims=True), jnp.sum(second_term, axis=1, keepdims=True)),
        "wide",
    )


def norm_forward(inputs, gain_shard, shift_shard):
    full_width = inputs.shape[1] * lax.axis_size("wide")
    total_sum, square_sum = row_totals(inputs, inputs * inputs)
    mean_row = total_sum / full_width
    inv_std = lax.rsqrt(square_sum / full_width - mean_row * mean_row + EPS)
    normed = (inputs - mean_row) * inv_std
    return (normed, inv_std, (normed * gain_shard + shift_shard).astype(BF))


def norm_backward(row_grads, normed, inv_std, gain_shard):
    full_width = row_grads.shape[1] * lax.axis_size("wide")
    scaled = row_grads * gain_shard
    first_sum, second_sum = row_totals(scaled, scaled * normed)
    return inv_std * (scaled - first_sum / full_width - normed * (second_sum / full_width))


def gather_tokens(values):
    return lax.all_gather(values, "wide", axis=0, tiled=True)


def gather_narrow(values):
    return lax.all_gather(values, "narrow", axis=0, tiled=True)


def sum_tokens(partial_value):
    return lax.psum_scatter(partial_value.astype(BF), "wide", scatter_dimension=0, tiled=True).astype(F32)


def sum_narrow(partial_value):
    return lax.psum_scatter(partial_value.astype(BF), "narrow", scatter_dimension=0, tiled=True).astype(F32)


def to_tokens(values):
    return lax.all_to_all(values, "wide", split_axis=0, concat_axis=1, tiled=True)


def to_features(values):
    return lax.all_to_all(values, "wide", split_axis=1, concat_axis=0, tiled=True)


def block_mask(starts):
    position = jnp.arange(starts.shape[0])
    return (position[None, :] <= position[:, None]) & (starts[:, None] == starts[None, :])


def split_heads(values):
    return values.reshape(values.shape[0], HEADS, HEAD)


def attend_forward(heads_all, allowed):
    score_scale = 1.0 / math.sqrt(HEAD)
    queries = split_heads(heads_all[:, 0])
    keys_part = split_heads(heads_all[:, 1])
    values_part = split_heads(heads_all[:, 2])
    scores = jnp.einsum("ihd,jhd->hij", queries, keys_part, preferred_element_type=F32) * score_scale
    log_total = jnp.log(jnp.sum(jnp.where(allowed, jnp.exp(scores), 0.0), axis=2, keepdims=True))
    attn_probs = jnp.where(allowed, jnp.exp(scores - log_total), 0.0).astype(BF)
    attended = jnp.einsum("hij,jhd->ihd", attn_probs, values_part, preferred_element_type=F32)
    return (attended.reshape(heads_all.shape[0], HEADS * HEAD).astype(BF), log_total)


def attend_backward(heads_all, allowed, log_total, attended_cot):
    score_scale = 1.0 / math.sqrt(HEAD)
    queries = split_heads(heads_all[:, 0])
    keys_part = split_heads(heads_all[:, 1])
    values_part = split_heads(heads_all[:, 2])
    scores = jnp.einsum("ihd,jhd->hij", queries, keys_part, preferred_element_type=F32) * score_scale
    probs_full = jnp.where(allowed, jnp.exp(scores - log_total), 0.0)
    cot_heads = split_heads(attended_cot)
    dprobs = jnp.einsum("ihd,jhd->hij", cot_heads, values_part, preferred_element_type=F32)
    row_delta = jnp.sum(probs_full * dprobs, axis=2, keepdims=True)
    score_cot = (probs_full * (dprobs - row_delta) * score_scale).astype(BF)
    query_grad = jnp.einsum("hij,jhd->ihd", score_cot, keys_part, preferred_element_type=F32)
    key_grad = jnp.einsum("hij,ihd->jhd", score_cot, queries, preferred_element_type=F32)
    value_grad = jnp.einsum("hij,ihd->jhd", probs_full.astype(BF), cot_heads, preferred_element_type=F32)
    stacked = jnp.stack([query_grad, key_grad, value_grad], axis=1)
    return stacked.reshape(heads_all.shape[0], 3, HEADS * HEAD)


MESH = pl.DeviceIdType.MESH
VMEM_LIMIT = 60 * 1024 * 1024
def params(collective_id):
    return pltpu.CompilerParams(
        collective_id=collective_id, has_side_effects=True, vmem_limit_bytes=VMEM_LIMIT
    )


def in_vmem(count):
    return [pl.BlockSpec(memory_space=pltpu.VMEM)] * count


def shape_of(shape, dtype):
    return jax.ShapeDtypeStruct(shape, dtype)


def square_peers():
    me = lax.axis_index("wide")
    return me, me + 1 - 2 * lax.rem(me, 2), lax.rem(me + 2, 4), 3 - me


def greet(peers, line=None):
    barrier = pltpu.get_barrier_semaphore()
    count = len(peers)
    for axis, peer in peers:
        pl.semaphore_signal(barrier, inc=1, device_id={axis: peer}, device_id_type=MESH)
    if line is not None:
        n, _, has_down, has_up = line
        for has, peer in ((has_down, n - 1), (has_up, n + 1)):

            @pl.when(has)
            def _():
                pl.semaphore_signal(barrier, inc=1, device_id={"narrow": peer}, device_id_type=MESH)

        count = count + has_down.astype(jnp.int32) + has_up.astype(jnp.int32)
    pl.semaphore_wait(barrier, count)


def remote(src, dst, send_sem, recv_sem, axis, peer):
    return pltpu.make_async_remote_copy(
        src_ref=src,
        dst_ref=dst,
        send_sem=send_sem,
        recv_sem=recv_sem,
        device_id={axis: peer},
        device_id_type=MESH,
    )


def line_sides():
    n, count = lax.axis_index("narrow"), lax.axis_size("narrow")
    return n, count, n > 0, n < count - 1


def halves(cols):
    first = cols // 256 * 128
    return (0, first), (first, cols - first)


class SquareGather:
    def __init__(self, items, send_sem, recv_sem):
        self.items, self.send_sem, self.recv_sem = items, send_sem, recv_sem
        self.me, xp, yp, self.dg = square_peers()
        self.ways = ((xp, yp), (yp, xp))
        self.core = lax.axis_index("dp")

    def place(self, i, chip):
        return self.items[i][1](chip * 2 + self.core)

    def copy(self, i, k):
        first, second = self.ways[i % 2]
        own = self.items[i][0]
        src, dst, axis, peer = {
            0: (own, self.me, "wide", first),
            1: (own, self.me, "wide", second),
            2: (own, self.me, "dp", 1 - self.core),
            3: (None, first, "wide", second),
            4: (None, first, "dp", 1 - self.core),
            5: (None, second, "dp", 1 - self.core),
            6: (None, self.dg, "dp", 1 - self.core),
        }[k]
        dst = self.place(i, dst)
        return remote(dst if src is None else src, dst, self.send_sem.at[i, k], self.recv_sem.at[i, k], axis, peer)

    def start(self):
        for k in range(3):
            for i in range(len(self.items)):
                self.copy(i, k).start()
        for i in range(len(self.items)):
            self.place(i, self.me)[...] = self.items[i][0][...]

    def relay(self, i):
        self.copy(i, 0).wait_recv()
        self.copy(i, 3).start()
        self.copy(i, 4).start()
        self.copy(i, 1).wait_recv()
        self.copy(i, 5).start()

    def finish(self):
        for i in range(len(self.items)):
            self.copy(i, 3).wait_recv()
            self.copy(i, 6).start()
        for i in range(len(self.items)):
            for k in (2, 4, 5, 6):
                self.copy(i, k).wait_recv()
            for k in range(7):
                self.copy(i, k).wait_send()


class LineGather:
    def __init__(self, own_ref, all_ref, send_sem, recv_sem, core_send=None, core_recv=None):
        self.own_ref, self.all_ref, self.send_sem, self.recv_sem = own_ref, all_ref, send_sem, recv_sem
        self.core_send, self.core_recv = core_send, core_recv
        self.core = lax.axis_index("dp")
        self.n, self.count, self.has_down, self.has_up = line_sides()

    def place(self, block):
        return self.all_ref.at[block] if self.core_send is None else self.all_ref.at[block, self.core]

    def copy(self, block, way, src=None):
        place = self.place(block)
        return remote(
            place if src is None else src,
            place,
            self.send_sem.at[way, block],
            self.recv_sem.at[block],
            "narrow",
            self.n + 1 - 2 * way,
        )

    def share(self, block, src=None):
        place = self.place(block)
        return remote(
            place if src is None else src, place, self.core_send.at[block], self.core_recv.at[block], "dp", 1 - self.core
        )

    def start(self):
        @pl.when(self.has_up)
        def _():
            self.copy(self.n, 0, self.own_ref).start()

        @pl.when(self.has_down)
        def _():
            self.copy(self.n, 1, self.own_ref).start()

        if self.core_send is not None:
            self.share(self.n, self.own_ref).start()
        self.place(self.n)[...] = self.own_ref[...]

    def step(self, step):
        below, above = self.n - step, self.n + step

        @pl.when(below >= 0)
        def _():
            self.copy(below, 0).wait_recv()

            @pl.when(self.has_up)
            def _():
                self.copy(below, 0).start()

            if self.core_send is not None:
                self.share(below).start()

        @pl.when(above < self.count)
        def _():
            self.copy(above, 1).wait_recv()

            @pl.when(self.has_down)
            def _():
                self.copy(above, 1).start()

            if self.core_send is not None:
                self.share(above).start()

    def finish(self):
        for step in range(self.count):
            below, above = self.n - step, self.n + step

            @pl.when((below >= 0) & self.has_up)
            def _():
                self.copy(below, 0).wait_send()

            @pl.when((above < self.count) & self.has_down)
            def _():
                self.copy(above, 1).wait_send()

        if self.core_send is not None:
            for block in range(self.count):
                self.share(block).wait()


def front_kernel(
    x_ref, dy_ref, gain_ref, shift_ref, vec_ref, bias_ref, wo_ref, wq_ref,
    norm_ref, stat_ref, xt_ref, dyt_ref, vecs_ref, biases_ref, wos_ref, wqs_ref,
    sums, all_sums, wo_parts, wo_row,
    send_sem, recv_sem, near_send, near_recv, line_send, line_recv, core_send, core_recv, square_send, square_recv,
):
    feats, tokens = x_ref.shape
    wide = 4
    block = tokens // wide
    me, xp, yp, dg = square_peers()
    peers = (xp, yp, dg)
    n, count = lax.axis_index("narrow"), lax.axis_size("narrow")
    others = [lax.rem(n + k, count) for k in range(1, count)]
    greet(
        [("wide", peer) for peer in peers]
        + [("narrow", peer) for peer in others]
        + [("dp", 1 - lax.axis_index("dp"))]
    )
    copies = []

    def send(src, dst, sems, k, j, axis, peer):
        copy = remote(src, dst, sems[0].at[k, j], sems[1].at[k, j], axis, peer)
        copy.start()
        copies.append(copy)

    near, across = (near_send, near_recv), (send_sem, recv_sem)
    for j, peer in enumerate(others):
        send(wo_ref, wo_parts.at[n], near, 0, j, "narrow", peer)
        send(bias_ref, biases_ref.at[n], near, 1, j, "narrow", peer)
    line = LineGather(wq_ref, wqs_ref, line_send, line_recv, core_send, core_recv)
    line.start()
    wo_parts[n] = wo_ref[...]
    biases_ref[n] = bias_ref[...]
    x = x_ref[...]
    sums[...] = jnp.zeros_like(sums)
    stat_ref[...] = jnp.zeros_like(stat_ref)
    sums[0:1, :] = jnp.sum(x, axis=0, keepdims=True)
    sums[1:2, :] = jnp.sum(x * x, axis=0, keepdims=True)
    for j, peer in enumerate(peers):
        send(sums, all_sums.at[me], across, 0, j, "wide", peer)
        send(vec_ref, vecs_ref.at[me], across, 1, j, "wide", peer)
    vecs_ref[me] = vec_ref[...]
    mine = pl.ds(me * feats, feats)
    for k, (src, dst) in enumerate(((x_ref, xt_ref), (dy_ref, dyt_ref))):
        for j, peer in enumerate(peers):
            theirs = pl.ds(pl.multiple_of(peer * block, 128), block)
            send(src.at[:, theirs], dst.at[mine, :], across, 2 + k, j, "wide", peer)
        dst[mine, :] = src[:, pl.ds(pl.multiple_of(me * block, 128), block)]
    for copy in copies[: 2 * (count - 1)]:
        copy.wait()
    part = wo_ref.shape[1]
    for k in range(count):
        wo_row[:, k * part : (k + 1) * part] = wo_parts[k]
    items = [
        (wo_row.at[:, pl.ds(*span)], lambda index, span=span: wos_ref.at[index, :, pl.ds(*span)])
        for span in halves(wo_row.shape[1])
    ]
    gather = SquareGather(items, square_send, square_recv)
    gather.start()
    rest = copies[2 * (count - 1) :]
    for copy in rest[:6]:
        copy.wait()
    total = sums[...]
    for peer in peers:
        total = total + all_sums[peer]
    width = feats * wide
    mean = total[0:1, :] / width
    inv = lax.rsqrt(total[1:2, :] / width - mean * mean + EPS)
    stat_ref[0:1, :] = mean
    stat_ref[1:2, :] = inv
    norm_ref[...] = ((x_ref[...] - mean) * inv * gain_ref[...] + shift_ref[...]).astype(BF)
    line.step(1)
    for copy in rest[6:]:
        copy.wait()
    line.step(2)
    gather.relay(0)
    gather.relay(1)
    for step in range(3, count):
        line.step(step)
    gather.finish()
    line.finish()


def front_stage(x, dy, gain, shift, vec, bias, wo, wq):
    feats, tokens = x.shape
    count = lax.axis_size("narrow")
    width = wo.shape[1] * count
    return pl.pallas_call(
        front_kernel,
        out_shape=(
            shape_of((feats, tokens), BF),
            shape_of((8, tokens), F32),
            shape_of((4 * feats, tokens // 4), F32),
            shape_of((4 * feats, tokens // 4), F32),
            shape_of((4,) + vec.shape, F32),
            shape_of((count,) + bias.shape, F32),
            shape_of((8, wo.shape[0], width), BF),
            shape_of((count, 2) + wq.shape, BF),
        ),
        in_specs=in_vmem(8),
        out_specs=tuple(in_vmem(8)),
        scratch_shapes=[
            pltpu.VMEM((8, tokens), F32),
            pltpu.VMEM((4, 8, tokens), F32),
            pltpu.VMEM((count,) + wo.shape, BF),
            pltpu.VMEM((wo.shape[0], width), BF),
            pltpu.SemaphoreType.DMA((4, 3)),
            pltpu.SemaphoreType.DMA((4, 3)),
            pltpu.SemaphoreType.DMA((2, count - 1)),
            pltpu.SemaphoreType.DMA((2, count - 1)),
            pltpu.SemaphoreType.DMA((2, count)),
            pltpu.SemaphoreType.DMA((count,)),
            pltpu.SemaphoreType.DMA((count,)),
            pltpu.SemaphoreType.DMA((count,)),
            pltpu.SemaphoreType.DMA((2, 7)),
            pltpu.SemaphoreType.DMA((2, 7)),
        ],
        compiler_params=params(1),
        cost_estimate=pl.CostEstimate(flops=10**10, bytes_accessed=60 * 10**6, transcendentals=0),
        name="front_stage",
    )(x, dy, gain, shift, vec, bias, wo, wq)


def qkv_kernel(
    norm_ref, w_ref, bias_ref, dy_ref, out_ref, dys_ref,
    acc, first_out, first_in, second_out, second_in, send_sem, recv_sem, line_send, line_recv,
):
    pieces, feats, cols = w_ref.shape
    tokens = norm_ref.shape[0]
    block = tokens // 4
    me, xp, yp, dg = square_peers()
    greet((("wide", xp), ("wide", yp)), line_sides())
    line = LineGather(dy_ref, dys_ref, line_send, line_recv)
    line.start()

    def rows(index):
        return pl.ds(pl.multiple_of(index * block, block), block)

    def ways(p):
        turn = lax.rem(p, 2)
        return xp * (1 - turn) + yp * turn, yp * (1 - turn) + xp * turn

    def first_copy(p):
        return remote(first_out.at[p], first_in.at[p], send_sem.at[0, p], recv_sem.at[0, p], "wide", ways(p)[0])

    def second_copy(p):
        return remote(second_out.at[p], second_in.at[p], send_sem.at[1, p], recv_sem.at[1, p], "wide", ways(p)[1])

    def issue(p, carry):
        acc[p] = dot(norm_ref[...], w_ref[p], 1, 0)
        first_out[p, 0] = acc[p, rows(ways(p)[0]), :].astype(BF)
        first_out[p, 1] = acc[p, rows(dg), :].astype(BF)
        first_copy(p).start()
        return carry

    lax.fori_loop(0, pieces, issue, 0)
    line.step(1)

    def middle(p, carry):
        first_copy(p).wait()
        second_out[p] = (acc[p, rows(ways(p)[1]), :] + first_in[p, 1].astype(F32)).astype(BF)
        second_copy(p).start()
        return carry

    lax.fori_loop(0, pieces // 2, middle, 0)
    line.step(2)
    lax.fori_loop(pieces // 2, pieces, middle, 0)
    for step in range(3, line.count):
        line.step(step)

    def last(p, carry):
        second_copy(p).wait()
        total = acc[p, rows(me), :] + first_in[p, 0].astype(F32) + second_in[p].astype(F32)
        out_ref[p] = (total + bias_ref[p]).astype(BF)
        return carry

    lax.fori_loop(0, pieces, last, 0)
    line.finish()


def qkv_stage(norm, w, bias, dy):
    count = lax.axis_size("narrow")
    pieces, feats, cols = w.shape
    tokens = norm.shape[0]
    block = tokens // 4
    return pl.pallas_call(
        qkv_kernel,
        out_shape=(shape_of((pieces, block, cols), BF), shape_of((count,) + dy.shape, BF)),
        in_specs=in_vmem(4),
        out_specs=tuple(in_vmem(2)),
        scratch_shapes=[
            pltpu.VMEM((pieces, tokens, cols), F32),
            pltpu.VMEM((pieces, 2, block, cols), BF),
            pltpu.VMEM((pieces, 2, block, cols), BF),
            pltpu.VMEM((pieces, block, cols), BF),
            pltpu.VMEM((pieces, block, cols), BF),
            pltpu.SemaphoreType.DMA((2, pieces)),
            pltpu.SemaphoreType.DMA((2, pieces)),
            pltpu.SemaphoreType.DMA((2, count)),
            pltpu.SemaphoreType.DMA((count,)),
        ],
        compiler_params=params(2),
        cost_estimate=pl.CostEstimate(flops=3 * 10**10, bytes_accessed=10**8, transcendentals=0),
        name="qkv_stage",
    )(norm, w, bias, dy)


def line_gather_kernel(own_ref, all_ref, send_sem, recv_sem):
    greet((), line_sides())
    line = LineGather(own_ref, all_ref, send_sem, recv_sem)
    line.start()
    for step in range(1, line.count):
        line.step(step)
    line.finish()


def line_gather(own):
    count = lax.axis_size("narrow")
    return pl.pallas_call(
        line_gather_kernel,
        out_shape=shape_of((count,) + own.shape, own.dtype),
        in_specs=in_vmem(1),
        out_specs=pl.BlockSpec(memory_space=pltpu.VMEM),
        scratch_shapes=[pltpu.SemaphoreType.DMA((2, count)), pltpu.SemaphoreType.DMA((count,))],
        compiler_params=params(4),
        cost_estimate=pl.CostEstimate(flops=2 * 10**10, bytes_accessed=7 * 10**7, transcendentals=0),
        name="line_gather",
    )(own)


def pair_kernel(count, own_ref, *refs):
    weight_refs, all_ref, whole_refs = refs[:count], refs[count], refs[count + 1 : 2 * count + 1]
    send_sem, recv_sem, line_send, line_recv = refs[2 * count + 1 :]
    me, xp, yp, dg = square_peers()
    greet((("wide", xp), ("wide", yp), ("dp", 1 - lax.axis_index("dp"))), line_sides())
    line = LineGather(own_ref, all_ref, line_send, line_recv)
    items = [
        (weight.at[:, pl.ds(*span)], lambda index, span=span, whole=whole: whole.at[index, :, pl.ds(*span)])
        for weight, whole in zip(weight_refs, whole_refs)
        for span in halves(weight.shape[1])
    ]
    gather = SquareGather(items, send_sem, recv_sem)
    line.start()
    gather.start()
    line.step(1)
    gather.relay(0)
    gather.relay(1)
    line.step(2)
    for i in range(2, len(items)):
        gather.relay(i)
    for step in range(3, line.count):
        line.step(step)
    gather.finish()
    line.finish()


def pair_stage(own, *weights):
    count = lax.axis_size("narrow")
    items = 2 * len(weights)
    return pl.pallas_call(
        functools.partial(pair_kernel, len(weights)),
        out_shape=(
            shape_of((count,) + own.shape, own.dtype),
            *(shape_of((8,) + weight.shape, weight.dtype) for weight in weights),
        ),
        in_specs=in_vmem(1 + len(weights)),
        out_specs=tuple(in_vmem(1 + len(weights))),
        scratch_shapes=[
            pltpu.SemaphoreType.DMA((items, 7)),
            pltpu.SemaphoreType.DMA((items, 7)),
            pltpu.SemaphoreType.DMA((2, count)),
            pltpu.SemaphoreType.DMA((count,)),
        ],
        compiler_params=params(7),
        cost_estimate=pl.CostEstimate(flops=2 * 10**10, bytes_accessed=7 * 10**7, transcendentals=0),
        name="pair_stage",
    )(own, *weights)


class SquareSum:
    def __init__(self, part_ref, bufs, sems):
        self.part_ref = part_ref
        self.core_in, self.half, self.first_out, self.first_in, self.second_out, self.second_in = bufs
        self.core_send, self.core_recv, self.send_sem, self.recv_sem = sems
        self.me, xp, yp, self.dg = square_peers()
        self.ways = ((xp, yp), (yp, xp))
        self.core = lax.axis_index("dp")
        self.spans = halves(part_ref.shape[2])

    def core_copy(self, chip):
        return remote(
            self.part_ref.at[chip * 2 + 1 - self.core],
            self.core_in.at[chip],
            self.core_send.at[chip],
            self.core_recv.at[chip],
            "dp",
            1 - self.core,
        )

    def first_copy(self, i, k):
        cols = pl.ds(*self.spans[i])
        return remote(
            self.first_out.at[k, :, cols],
            self.first_in.at[k, :, cols],
            self.send_sem.at[i, k],
            self.recv_sem.at[i, k],
            "wide",
            self.ways[i][0],
        )

    def second_copy(self, i):
        cols = pl.ds(*self.spans[i])
        return remote(
            self.second_out.at[:, cols],
            self.second_in.at[:, cols],
            self.send_sem.at[i, 2],
            self.recv_sem.at[i, 2],
            "wide",
            self.ways[i][1],
        )

    def start(self):
        for chip in range(4):
            self.core_copy(chip).start()

    def issue(self):
        for chip in range(4):
            self.core_copy(chip).wait()
            total = self.part_ref[chip * 2 + self.core].astype(F32) + self.core_in[chip].astype(F32)
            self.half[chip] = total.astype(BF)
        for i, (at, size) in enumerate(self.spans):
            for k, chip in enumerate((self.ways[i][0], self.dg)):
                self.first_out[k, :, at : at + size] = self.half[chip, :, at : at + size]
                self.first_copy(i, k).start()

    def middle(self):
        for i, (at, size) in enumerate(self.spans):
            self.first_copy(i, 1).wait()
            total = self.half[self.ways[i][1], :, at : at + size].astype(F32)
            total = total + self.first_in[1, :, at : at + size].astype(F32)
            self.second_out[:, at : at + size] = total.astype(BF)
            self.second_copy(i).start()

    def finish(self, out_ref):
        for i, (at, size) in enumerate(self.spans):
            self.first_copy(i, 0).wait()
            self.second_copy(i).wait()
            total = self.half[self.me, :, at : at + size].astype(F32)
            total = total + self.first_in[0, :, at : at + size].astype(F32)
            out_ref[:, at : at + size] = total + self.second_in[:, at : at + size].astype(F32)


def square_sum_scratch(rows, cols):
    return [
        pltpu.VMEM((4, rows, cols), BF),
        pltpu.VMEM((4, rows, cols), BF),
        pltpu.VMEM((2, rows, cols), BF),
        pltpu.VMEM((2, rows, cols), BF),
        pltpu.VMEM((rows, cols), BF),
        pltpu.VMEM((rows, cols), BF),
        pltpu.SemaphoreType.DMA((4,)),
        pltpu.SemaphoreType.DMA((4,)),
        pltpu.SemaphoreType.DMA((2, 3)),
        pltpu.SemaphoreType.DMA((2, 3)),
    ]


def back_kernel(
    cot_ref, norm_ref, w_ref, wo_ref,
    grad_ref, wq_out, wo_out,
    cots, full, other, core_in, leave, arrive, wo_row, wo_leave, wo_arrive,
    send_sem, recv_sem, core_send, core_recv, line_send, line_recv, near_send, near_recv, share_send, share_recv,
    *square,
):
    pieces, block, cols = cot_ref.shape
    me, xp, yp, dg = square_peers()
    n, count, has_down, has_up = line_sides()
    core = lax.axis_index("dp")
    others = [lax.rem(n + k, count) for k in range(1, count)]
    greet(
        [("wide", xp), ("wide", yp), ("dp", 1 - core)] + [("narrow", peer) for peer in others]
    )
    spans = halves(cols)
    ways = ((xp, yp), (yp, xp))
    rows_half = core_in.shape[1]

    def order(i):
        odd = lax.rem(i, 2)
        return (1 - odd) * (i // 2) + odd * (pieces - 1 - i // 2)

    def rows(index):
        return pl.ds(pl.multiple_of(index * block, block), block)

    def spread(i, h, k):
        p = order(i)
        span = pl.ds(*spans[h])
        first, second = ways[h]
        place = cots.at[p, rows(first if k == 2 else me), span]
        src = place if k == 2 else cot_ref.at[p, :, span]
        return remote(
            src, place, send_sem.at[h, k, p], recv_sem.at[h, k, p], "wide", first if k == 0 else second
        )

    def own(i):
        for h in range(2):
            for k in range(2):
                spread(i, h, k).start()
        p = order(i)
        cots[p, rows(me), :] = cot_ref[p]

    def core_copy(p):
        return remote(other.at[p], core_in.at[p], core_send.at[p], core_recv.at[p], "dp", 1 - core)

    def line_copy(way, p):
        return remote(
            leave.at[p], arrive.at[way, p], line_send.at[p], line_recv.at[way, p], "narrow", n + 1 - 2 * way
        )

    own_rows = pl.ds(pl.multiple_of(core * rows_half, 8), rows_half)
    sibling_rows = pl.ds(pl.multiple_of((1 - core) * rows_half, 8), rows_half)
    square_sum = SquareSum(wo_ref, square[:6], square[6:])
    own(0)
    own(1)
    square_sum.start()
    grad_ref[...] = jnp.zeros_like(grad_ref)

    def turn(p):
        core_copy(p).wait()
        mine = full[p, own_rows, :] + core_in[p].astype(F32)
        full[p, own_rows, :] = mine

        def pass_on(way, sends, joins):
            @pl.when(sends & joins)
            def _():
                line_copy(way, p).wait_recv()
                leave[p] = (full[p, own_rows, :] + arrive[way, p].astype(F32)).astype(BF)
                line_copy(way, p).start()

            @pl.when(sends & jnp.logical_not(joins))
            def _():
                leave[p] = full[p, own_rows, :].astype(BF)
                line_copy(way, p).start()

        pass_on(0, n < p, has_down)
        pass_on(1, n > p, has_up)

    def body(i, carry):
        @pl.when(i < pieces)
        def _():
            for h in range(2):
                spread(i, h, 0).wait_recv()
                spread(i, h, 2).start()

        @pl.when(i + 2 < pieces)
        def _():
            own(i + 2)

        @pl.when((i >= 1) & (i <= pieces))
        def _():
            p = order(i - 1)
            for h in range(2):
                spread(i - 1, h, 1).wait_recv()
                spread(i - 1, h, 2).wait_recv()
            full[p] = dot(norm_ref[...], cots[p], 1, 0)
            other[p] = full[p, sibling_rows, :].astype(BF)
            core_copy(p).start()
            grad_ref[...] += dot(w_ref[p], cots[p], 1, 1)

        @pl.when(i >= 2)
        def _():
            turn(order(i - 2))

        @pl.when(i == pieces - 1)
        def _():
            square_sum.issue()

        return carry

    lax.fori_loop(0, pieces + 2, body, 0)
    square_sum.middle()
    square_sum.finish(wo_row)
    part = wo_leave.shape[2]
    for k in range(count):
        wo_leave[k] = wo_row[:, k * part : (k + 1) * part].astype(BF)
    near = []
    for j, peer in enumerate(others):
        copy = remote(wo_leave.at[peer], wo_arrive.at[n], near_send.at[j], near_recv.at[j], "narrow", peer)
        copy.start()
        near.append(copy)
    total = full[n, own_rows, :]
    for way, joins in ((0, has_down), (1, has_up)):

        @pl.when(joins)
        def _():
            line_copy(way, n).wait_recv()
            full[n, own_rows, :] += arrive[way, n].astype(F32)

    wq_out[core] = full[n, own_rows, :]
    share_wq = remote(wq_out.at[core], wq_out.at[core], share_send.at[0], share_recv.at[0], "dp", 1 - core)
    share_wq.start()
    for copy in near:
        copy.wait()
    wo_total = wo_leave[n].astype(F32)
    for peer in others:
        wo_total = wo_total + wo_arrive[peer].astype(F32)
    wo_out[core] = wo_total
    share_wo = remote(wo_out.at[core], wo_out.at[core], share_send.at[1], share_recv.at[1], "dp", 1 - core)
    share_wo.start()

    def drain(i, carry):
        for h in range(2):
            for k in range(3):
                spread(i, h, k).wait_send()
        p = order(i)

        @pl.when(n < p)
        def _():
            line_copy(0, p).wait_send()

        @pl.when(n > p)
        def _():
            line_copy(1, p).wait_send()

        return carry

    lax.fori_loop(0, pieces, drain, 0)
    share_wq.wait()
    share_wo.wait()


def back_stage(cot, norm, w, wo):
    pieces, block, cols = cot.shape
    count = lax.axis_size("narrow")
    feats, tokens = norm.shape
    rows, wo_cols = wo.shape[1:]
    half = feats // 2
    part = wo_cols // count
    return pl.pallas_call(
        back_kernel,
        out_shape=(
            shape_of((feats, tokens), F32),
            shape_of((2, half, cols), F32),
            shape_of((2, rows, part), F32),
        ),
        in_specs=in_vmem(4),
        out_specs=tuple(in_vmem(3)),
        scratch_shapes=[
            pltpu.VMEM((pieces, tokens, cols), BF),
            pltpu.VMEM((pieces, feats, cols), F32),
            pltpu.VMEM((pieces, half, cols), BF),
            pltpu.VMEM((pieces, half, cols), BF),
            pltpu.VMEM((pieces, half, cols), BF),
            pltpu.VMEM((2, pieces, half, cols), BF),
            pltpu.VMEM((rows, wo_cols), F32),
            pltpu.VMEM((count, rows, part), BF),
            pltpu.VMEM((count, rows, part), BF),
            pltpu.SemaphoreType.DMA((2, 3, pieces)),
            pltpu.SemaphoreType.DMA((2, 3, pieces)),
            pltpu.SemaphoreType.DMA((pieces,)),
            pltpu.SemaphoreType.DMA((pieces,)),
            pltpu.SemaphoreType.DMA((pieces,)),
            pltpu.SemaphoreType.DMA((2, pieces)),
            pltpu.SemaphoreType.DMA((count - 1,)),
            pltpu.SemaphoreType.DMA((count - 1,)),
            pltpu.SemaphoreType.DMA((2,)),
            pltpu.SemaphoreType.DMA((2,)),
        ]
        + square_sum_scratch(rows, wo_cols),
        compiler_params=params(3),
        cost_estimate=pl.CostEstimate(flops=4 * 10**10, bytes_accessed=10**8, transcendentals=0),
        name="back_stage",
    )(cot, norm, w, wo)


TOKEN_TERMS = 5


def final_kernel(
    x_ref, stat_ref, grad_ref, resid_ref, gain_ref, sums_ref, wide_ref, feat_ref, wf_ref, wp_ref,
    out_ref, wide_out, feat_out, wf_out, wp_out,
    all_sums, wide_in, wide_mid, line_wide, line_feat, wide_two, feat_two, last_wide, last_feat,
    wf_in, wp_in, send_sem, recv_sem, line_send, line_recv, core_send, core_recv,
):
    me, xp, yp, dg = square_peers()
    n, count = lax.axis_index("narrow"), lax.axis_size("narrow")
    core = lax.axis_index("dp")
    peers = (xp, yp, dg)
    others = [lax.rem(n + k, count) for k in range(1, count)]
    greet(
        [("wide", peer) for peer in peers] + [("narrow", peer) for peer in others] + [("dp", 1 - core)]
    )
    shares = []
    for k, (src, dst) in enumerate(((wf_ref, wf_in), (wp_ref, wp_in))):
        copy = remote(src, dst, core_send.at[2 + k], core_recv.at[2 + k], "dp", 1 - core)
        copy.start()
        shares.append(copy)
    square = []
    for j, peer in enumerate(peers):
        for k, (src, dst) in enumerate(((sums_ref, all_sums), (wide_ref, wide_in))):
            copy = remote(src, dst.at[me], send_sem.at[k, j], recv_sem.at[k, j], "wide", peer)
            copy.start()
            square.append(copy)
    for copy in square:
        copy.wait()
    total = wide_ref[...]
    for peer in peers:
        total = total + wide_in[peer]
    wide_mid[...] = total
    line = []
    for j, peer in enumerate(others):
        for k, (src, dst) in enumerate(((wide_mid, line_wide), (feat_ref, line_feat))):
            copy = remote(src, dst.at[n], line_send.at[k, j], line_recv.at[k, j], "narrow", peer)
            copy.start()
            line.append(copy)
    sums = sums_ref[...]
    for peer in peers:
        sums = sums + all_sums[peer]
    width = x_ref.shape[0] * 4
    inv = stat_ref[1:2, :]
    normed = (x_ref[...] - stat_ref[0:1, :]) * inv
    scaled = grad_ref[...] * gain_ref[...]
    out_ref[...] = resid_ref[...] + inv * (scaled - sums[0:1, :] / width - normed * (sums[1:2, :] / width))
    wf_out[core] = wf_ref[...].astype(F32)
    wp_out[core] = wp_ref[...].astype(F32)
    for copy in shares:
        copy.wait()
    wf_out[1 - core] = wf_in[...].astype(F32)
    wp_out[1 - core] = wp_in[...].astype(F32)
    for copy in line:
        copy.wait()
    feat_total = feat_ref[...]
    shared = lax.broadcasted_iota(jnp.int32, total.shape, 0) < TOKEN_TERMS
    for peer in others:
        total = total + jnp.where(shared, line_wide[peer], 0.0)
        feat_total = feat_total + line_feat[peer]
    wide_two[...] = total
    feat_two[...] = feat_total
    cores = []
    for k, (src, dst) in enumerate(((wide_two, last_wide), (feat_two, last_feat))):
        copy = remote(src, dst, core_send.at[k], core_recv.at[k], "dp", 1 - core)
        copy.start()
        cores.append(copy)
    for copy in cores:
        copy.wait()
    wide_out[...] = total + last_wide[...]
    feat_out[...] = feat_total + last_feat[...]


def final_stage(x, stats, grad, resid, gain, sums, wide_terms, feat_terms, wf, wp):
    count = lax.axis_size("narrow")
    return pl.pallas_call(
        final_kernel,
        out_shape=(
            shape_of(x.shape, F32),
            shape_of(wide_terms.shape, F32),
            shape_of(feat_terms.shape, F32),
            shape_of((2,) + wf.shape, F32),
            shape_of((2,) + wp.shape, F32),
        ),
        in_specs=in_vmem(10),
        out_specs=tuple(in_vmem(5)),
        scratch_shapes=[
            pltpu.VMEM((4,) + sums.shape, F32),
            pltpu.VMEM((4,) + wide_terms.shape, F32),
            pltpu.VMEM(wide_terms.shape, F32),
            pltpu.VMEM((count,) + wide_terms.shape, F32),
            pltpu.VMEM((count,) + feat_terms.shape, F32),
            pltpu.VMEM(wide_terms.shape, F32),
            pltpu.VMEM(feat_terms.shape, F32),
            pltpu.VMEM(wide_terms.shape, F32),
            pltpu.VMEM(feat_terms.shape, F32),
            pltpu.VMEM(wf.shape, BF),
            pltpu.VMEM(wp.shape, BF),
            pltpu.SemaphoreType.DMA((2, 3)),
            pltpu.SemaphoreType.DMA((2, 3)),
            pltpu.SemaphoreType.DMA((2, count - 1)),
            pltpu.SemaphoreType.DMA((2, count - 1)),
            pltpu.SemaphoreType.DMA((4,)),
            pltpu.SemaphoreType.DMA((4,)),
        ],
        compiler_params=params(8),
        cost_estimate=pl.CostEstimate(flops=10**9, bytes_accessed=2 * 10**7, transcendentals=0),
        name="final_stage",
    )(x, stats, grad, resid, gain, sums, wide_terms, feat_terms, wf, wp)


def as_rows(rows):
    return jnp.concatenate([jnp.stack(rows), jnp.zeros((8 - len(rows), rows[0].shape[0]), F32)])


def own_half(values, axis):
    half = values.shape[axis] // lax.axis_size("dp")
    return lax.dynamic_slice_in_dim(values, lax.axis_index("dp") * half, half, axis)


def local(
    block_input,
    block_cotangent,
    seq_start,
    ln1_gain,
    ln1_shift,
    w_qkv,
    b_qv,
    w_out,
    b_out,
    ln2_gain,
    ln2_shift,
    w_fc,
    b_fc,
    w_proj,
    b_proj,
):
    cores, wide, narrow = lax.axis_size("dp"), lax.axis_size("wide"), lax.axis_size("narrow")
    w_index, n_index = lax.axis_index("wide"), lax.axis_index("narrow")
    feats, part = w_qkv.shape[0], w_qkv.shape[2]
    width = feats * wide
    hid = w_fc.shape[1]

    perm = []
    for w in range(wide):
        for n in range(narrow):
            block = n * wide + w
            perm.append((block, w * narrow + n))
    starts = lax.ppermute(seq_start, ("wide", "narrow"), perm)[0]
    allowed = block_mask(starts)

    wq_half = own_half(w_qkv, 0).astype(BF).reshape(-1, 3 * part)
    wo_half, wf_half, wp_half = (own_half(w, 0).astype(BF) for w in (w_out, w_fc, w_proj))

    def three(biases):
        zeros = jnp.zeros((narrow, 1, part), F32)
        return jnp.concatenate([biases[:, None, 0], zeros, biases[:, None, 1]], axis=2)

    rows_input = block_input.T
    rows_cot = block_cotangent.T
    square = wide == 4 and cores == 2
    if square:
        norm_t, stats, x_tok, dy_tok, vecs, biases, wo_all, wq_all = front_stage(
            block_input,
            block_cotangent,
            ln1_gain[:, None],
            ln1_shift[:, None],
            as_rows([b_out, ln2_gain, ln2_shift]),
            as_rows([b_qv[0], b_qv[1]]),
            wo_half,
            wq_half,
        )
        x_tok, dy_tok = x_tok.T, dy_tok.T
        wo_all = wo_all.reshape(width, width)
        wq_all = wq_all.reshape(narrow, feats, 3 * part)
        b_out_full, gain_two_full, shift_two_full = (vecs[:, i].reshape(width) for i in range(3))
        qkv_rows, cot_all = qkv_stage(norm_t.T, wq_all, three(biases), dy_tok.astype(BF))
        cot_all = cot_all.reshape(-1, width)
    else:
        wq_all = lax.all_gather(wq_half, ("narrow", "dp"), axis=0, tiled=True).reshape(narrow, feats, 3 * part)
        wo_mine = lax.all_gather(wo_half, "narrow", axis=1, tiled=True)
        wo_all = lax.all_gather(wo_mine, ("wide", "dp"), axis=0, tiled=True)
        wf_all = lax.all_gather(wf_half, ("wide", "dp"), axis=0, tiled=True)
        wp_all = lax.all_gather(wp_half, ("wide", "dp"), axis=0, tiled=True)
        bias_three = three(lax.all_gather(b_qv, "narrow", axis=0))
        b_out_full, gain_two_full, shift_two_full = lax.all_gather(
            jnp.stack([b_out, ln2_gain, ln2_shift]), "wide", axis=1, tiled=True
        )
        x_tok = to_tokens(rows_input)
        dy_tok = to_tokens(rows_cot)
        normed_one, inv_one, norm_one = norm_forward(rows_input, ln1_gain, ln1_shift)
        qkv_part = jnp.einsum("tk,nkc->tnc", norm_one, wq_all, preferred_element_type=F32)
        qkv_rows = sum_tokens(qkv_part).transpose(1, 0, 2)
        qkv_rows = (qkv_rows + bias_three).astype(BF)
        cot_all = gather_narrow(dy_tok.astype(BF))
    heads_all = qkv_rows.reshape(narrow, -1, 3, part).transpose(1, 2, 0, 3).reshape(-1, 3, width)
    attended, log_total = attend_forward(heads_all, allowed)
    residual = x_tok + dot(attended, wo_all, 1, 1) + b_out_full
    mean_two = jnp.mean(residual, axis=1, keepdims=True)
    inv_two = lax.rsqrt(jnp.mean(residual * residual, axis=1, keepdims=True) - mean_two * mean_two + EPS)
    normed_two = (residual - mean_two) * inv_two
    norm_two = (normed_two * gain_two_full + shift_two_full).astype(BF)
    if square:
        norm_two_all, wf_all, wp_all = pair_stage(norm_two, wf_half, wp_half)
        norm_two_all = norm_two_all.reshape(-1, width)
        wf_all, wp_all = wf_all.reshape(width, hid), wp_all.reshape(width, hid)
    else:
        norm_two_all = line_gather(norm_two).reshape(-1, width)
    pre_act = dot(norm_two_all, wf_all, 1, 0) + b_fc
    hidden = gelu_value(pre_act).astype(BF)
    out_tok = residual + sum_narrow(dot(hidden, wp_all, 1, 1))
    output_rows = to_features(out_tok) + b_proj

    pre_grad = dot(cot_all, wp_all, 1, 0) * gelu_slope(pre_act)
    pre_cot = pre_grad.astype(BF)
    norm_two_grad = sum_narrow(dot(pre_cot, wf_all, 1, 1))

    def reduce_wide(grad):
        total = lax.psum_scatter(grad.astype(BF), ("wide", "dp"), scatter_dimension=0, tiled=True)
        return total

    def share(total):
        return lax.all_gather(total, "dp", axis=0, tiled=True).astype(F32)

    wp_grad = reduce_wide(dot(cot_all, hidden, 0, 0))
    wf_grad = reduce_wide(dot(norm_two_all, pre_cot, 0, 0))

    scaled = norm_two_grad * gain_two_full
    mean_scaled = jnp.mean(scaled, axis=1, keepdims=True)
    mean_cross = jnp.mean(scaled * normed_two, axis=1, keepdims=True)
    resid_grad = dy_tok + inv_two * (scaled - mean_scaled - normed_two * mean_cross)
    resid_cot = resid_grad.astype(BF)
    attended_cot = dot(resid_cot, wo_all, 1, 0).astype(BF)
    wo_grad = dot(resid_cot, attended, 0, 0).astype(BF)

    qkv_grad = attend_backward(heads_all, allowed, log_total, attended_cot)
    qkv_cot = qkv_grad.astype(BF).reshape(-1, 3, narrow, part).transpose(2, 0, 1, 3)
    qkv_cot = qkv_cot.reshape(narrow, -1, 3 * part)
    if square:
        norm_one_grad, grad_w_qkv, grad_w_out = back_stage(
            qkv_cot, norm_t, wq_all, wo_grad.reshape(2 * wide, -1, width)
        )
        grad_w_qkv = grad_w_qkv.reshape(feats, 3, part)
        grad_w_out = grad_w_out.reshape(feats, part)
    else:
        qkv_cot_all = lax.all_gather(qkv_cot, "wide", axis=1, tiled=True)
        wq_grad = jnp.einsum("tk,ntc->nkc", norm_one, qkv_cot_all, preferred_element_type=F32).astype(BF)
        wq_grad = lax.psum_scatter(
            wq_grad.reshape(narrow * feats, 3 * part), ("narrow", "dp"), scatter_dimension=0, tiled=True
        )
        grad_w_qkv = share(wq_grad).reshape(feats, 3, part)
        norm_one_grad = jnp.einsum("nkc,ntc->kt", wq_all, qkv_cot_all, preferred_element_type=F32)
        wo_grad = lax.psum_scatter(reduce_wide(wo_grad), "narrow", scatter_dimension=1, tiled=True)
        grad_w_out = share(wo_grad)

    resid_back = to_features(resid_grad).T
    qkv_sums = jnp.sum(qkv_grad, axis=0)
    wide_terms = as_rows(
        [
            qkv_sums[0],
            qkv_sums[2],
            jnp.sum(resid_grad, axis=0),
            jnp.sum(norm_two_grad * normed_two, axis=0),
            jnp.sum(norm_two_grad, axis=0),
        ]
    )
    fc_terms = jnp.sum(pre_grad, axis=0)
    if square:
        normed = (block_input - stats[0:1]) * stats[1:2]
        scaled = norm_one_grad * ln1_gain[:, None]
        sums = as_rows([jnp.sum(scaled, axis=0), jnp.sum(scaled * normed, axis=0)])
        feat_terms = as_rows(
            [jnp.sum(norm_one_grad * normed, axis=1), jnp.sum(norm_one_grad, axis=1), jnp.sum(block_cotangent, axis=1)]
        )
        span = max(width, hid)
        packed = jnp.zeros((8, span), F32)
        packed = packed.at[:, :width].set(wide_terms).at[TOKEN_TERMS, :hid].set(fc_terms)
        grad_input, packed_sum, feat_sum, grad_w_fc, grad_w_proj = final_stage(
            block_input,
            stats,
            norm_one_grad,
            resid_back,
            ln1_gain[:, None],
            sums,
            packed,
            feat_terms,
            wf_grad,
            wp_grad,
        )
        grad_w_fc, grad_w_proj = grad_w_fc.reshape(w_fc.shape), grad_w_proj.reshape(w_proj.shape)
        token_sum = packed_sum[:TOKEN_TERMS, :width]
        grad_b_fc = packed_sum[TOKEN_TERMS, :hid]
        gain_one, shift_one, proj_bias = feat_sum[0], feat_sum[1], feat_sum[2]
    else:
        grad_w_proj, grad_w_fc = share(wp_grad), share(wf_grad)
        norm_one_grad = norm_one_grad.T
        grad_input = (resid_back.T + norm_backward(norm_one_grad, normed_one, inv_one, ln1_gain)).T
        feature_terms = jnp.stack(
            [
                jnp.sum(norm_one_grad * normed_one, axis=0),
                jnp.sum(norm_one_grad, axis=0),
                jnp.sum(rows_cot, axis=0),
            ]
        )
        feature_full = lax.dynamic_update_slice_in_dim(
            jnp.zeros((3, width), F32), feature_terms, w_index * feats, 1
        )
        fc_full = lax.dynamic_update_slice_in_dim(jnp.zeros((narrow * hid,), F32), fc_terms, n_index * hid, 0)
        token_sum, feature_sum, fc_sum = lax.psum((wide_terms, feature_full, fc_full), ("dp", "wide", "narrow"))
        gain_one, shift_one, proj_bias = lax.dynamic_slice_in_dim(feature_sum, w_index * feats, feats, 1)
        grad_b_fc = lax.dynamic_slice_in_dim(fc_sum, n_index * hid, hid, 0)
    grad_b_qv = lax.dynamic_slice_in_dim(token_sum[:2], n_index * part, part, 1)
    out_bias, gain_two, shift_two = lax.dynamic_slice_in_dim(token_sum[2:5], w_index * feats, feats, 1)
    return (
        output_rows.T,
        grad_input,
        gain_one,
        shift_one,
        grad_w_qkv,
        grad_b_qv,
        grad_w_out,
        out_bias,
        gain_two,
        shift_two,
        grad_w_fc,
        grad_b_fc,
        grad_w_proj,
        proj_bias,
    )


def solution(mesh):
    return jax.shard_map(
        local,
        mesh=mesh,
        in_specs=(
            P("wide", ("dp", "narrow")),
            P("wide", ("dp", "narrow")),
            P(("dp", "wide", "narrow"), None),
            P("wide"),
            P("wide"),
            P("wide", None, "narrow"),
            P(None, "narrow"),
            P("wide", "narrow"),
            P("wide"),
            P("wide"),
            P("wide"),
            P("wide", "narrow"),
            P("narrow"),
            P("wide", "narrow"),
            P("wide"),
        ),
        out_specs=(
            P("wide", ("dp", "narrow")),
            P("wide", ("dp", "narrow")),
            P("wide"),
            P("wide"),
            P("wide", None, "narrow"),
            P(None, "narrow"),
            P("wide", "narrow"),
            P("wide"),
            P("wide"),
            P("wide"),
            P("wide", "narrow"),
            P("narrow"),
            P("wide", "narrow"),
            P("wide"),
        ),
        check_vma=False,
    )
```

```python
import functools
import math

import jax
import jax.numpy as jnp
from jax import lax
from jax.experimental import pallas as pl
from jax.experimental.pallas import tpu as pltpu
from jax.sharding import PartitionSpec as P

HEADS = 25
HEAD = 64

EPS = 1e-05
GELU_C = math.sqrt(2.0 / math.pi)
BF = jnp.bfloat16
F32 = jnp.float32


def gelu_value(pre_act):
    inner = GELU_C * (pre_act + 0.044715 * pre_act * pre_act * pre_act)
    return 0.5 * pre_act * (1.0 + jnp.tanh(inner))


def gelu_slope(pre_act):
    tanh_part = jnp.tanh(GELU_C * (pre_act + 0.044715 * pre_act * pre_act * pre_act))
    return 0.5 * (1.0 + tanh_part) + 0.5 * pre_act * (1.0 - tanh_part * tanh_part) * GELU_C * (
        1.0 + 3.0 * 0.044715 * pre_act * pre_act
    )


def dot(a, b, ca, cb):
    return lax.dot_general(a, b, (((ca,), (cb,)), ((), ())), preferred_element_type=F32)


def row_totals(first_term, second_term):
    return lax.psum(
        (jnp.sum(first_term, axis=1, keepdims=True), jnp.sum(second_term, axis=1, keepdims=True)),
        "wide",
    )


def norm_forward(inputs, gain_shard, shift_shard):
    full_width = inputs.shape[1] * lax.axis_size("wide")
    total_sum, square_sum = row_totals(inputs, inputs * inputs)
    mean_row = total_sum / full_width
    inv_std = lax.rsqrt(square_sum / full_width - mean_row * mean_row + EPS)
    normed = (inputs - mean_row) * inv_std
    return (normed, inv_std, (normed * gain_shard + shift_shard).astype(BF))


def norm_backward(row_grads, normed, inv_std, gain_shard):
    full_width = row_grads.shape[1] * lax.axis_size("wide")
    scaled = row_grads * gain_shard
    first_sum, second_sum = row_totals(scaled, scaled * normed)
    return inv_std * (scaled - first_sum / full_width - normed * (second_sum / full_width))


def gather_narrow(values):
    return lax.all_gather(values, "narrow", axis=1, tiled=True)


def sum_tokens(partial_value):
    return lax.psum_scatter(partial_value.astype(BF), "wide", scatter_dimension=0, tiled=True).astype(F32)


def sum_narrow(partial_value):
    return lax.psum_scatter(partial_value.astype(BF), "narrow", scatter_dimension=1, tiled=True).astype(F32)


def to_tokens(values):
    return lax.all_to_all(values, "wide", split_axis=1, concat_axis=0, tiled=True)


def to_features(values):
    return lax.all_to_all(values, "wide", split_axis=0, concat_axis=1, tiled=True)


def block_mask(starts):
    position = jnp.arange(starts.shape[0])
    return (position[None, :] <= position[:, None]) & (starts[:, None] == starts[None, :])


def split_heads(values):
    return values.reshape(values.shape[0], HEADS, HEAD)


def attend_forward(heads_all, allowed):
    score_scale = 1.0 / math.sqrt(HEAD)
    queries = split_heads(heads_all[:, 0])
    keys_part = split_heads(heads_all[:, 1])
    values_part = split_heads(heads_all[:, 2])
    scores = jnp.einsum("ihd,jhd->hij", queries, keys_part, preferred_element_type=F32) * score_scale
    log_total = jnp.log(jnp.sum(jnp.where(allowed, jnp.exp(scores), 0.0), axis=2, keepdims=True))
    attn_probs = jnp.where(allowed, jnp.exp(scores - log_total), 0.0).astype(BF)
    attended = jnp.einsum("hij,jhd->ihd", attn_probs, values_part, preferred_element_type=F32)
    return (attended.reshape(heads_all.shape[0], HEADS * HEAD).astype(BF), log_total)


def attend_backward(heads_all, allowed, log_total, attended_cot):
    score_scale = 1.0 / math.sqrt(HEAD)
    queries = split_heads(heads_all[:, 0])
    keys_part = split_heads(heads_all[:, 1])
    values_part = split_heads(heads_all[:, 2])
    scores = jnp.einsum("ihd,jhd->hij", queries, keys_part, preferred_element_type=F32) * score_scale
    probs_full = jnp.where(allowed, jnp.exp(scores - log_total), 0.0)
    cot_heads = split_heads(attended_cot)
    dprobs = jnp.einsum("ihd,jhd->hij", cot_heads, values_part, preferred_element_type=F32)
    row_delta = jnp.sum(probs_full * dprobs, axis=2, keepdims=True)
    score_cot = (probs_full * (dprobs - row_delta) * score_scale).astype(BF)
    query_grad = jnp.einsum("hij,jhd->ihd", score_cot, keys_part, preferred_element_type=F32)
    key_grad = jnp.einsum("hij,ihd->jhd", score_cot, queries, preferred_element_type=F32)
    value_grad = jnp.einsum("hij,ihd->jhd", probs_full.astype(BF), cot_heads, preferred_element_type=F32)
    stacked = jnp.stack([query_grad, key_grad, value_grad], axis=1)
    return stacked.reshape(heads_all.shape[0], 3, HEADS * HEAD)


MESH = pl.DeviceIdType.MESH
VMEM_LIMIT = 60 * 1024 * 1024
def params(collective_id):
    return pltpu.CompilerParams(
        collective_id=collective_id, has_side_effects=True, vmem_limit_bytes=VMEM_LIMIT
    )


def in_vmem(count):
    return [pl.BlockSpec(memory_space=pltpu.VMEM)] * count


def shape_of(shape, dtype):
    return jax.ShapeDtypeStruct(shape, dtype)


def square_peers():
    me = lax.axis_index("wide")
    return me, me + 1 - 2 * lax.rem(me, 2), lax.rem(me + 2, 4), 3 - me


def greet(peers, line=None):
    barrier = pltpu.get_barrier_semaphore()
    count = len(peers)
    for axis, peer in peers:
        pl.semaphore_signal(barrier, inc=1, device_id={axis: peer}, device_id_type=MESH)
    if line is not None:
        n, _, has_down, has_up = line
        for has, peer in ((has_down, n - 1), (has_up, n + 1)):

            @pl.when(has)
            def _():
                pl.semaphore_signal(barrier, inc=1, device_id={"narrow": peer}, device_id_type=MESH)

        count = count + has_down.astype(jnp.int32) + has_up.astype(jnp.int32)
    pl.semaphore_wait(barrier, count)


def remote(src, dst, send_sem, recv_sem, axis, peer):
    return pltpu.make_async_remote_copy(
        src_ref=src,
        dst_ref=dst,
        send_sem=send_sem,
        recv_sem=recv_sem,
        device_id={axis: peer},
        device_id_type=MESH,
    )


def line_sides():
    n, count = lax.axis_index("narrow"), lax.axis_size("narrow")
    return n, count, n > 0, n < count - 1


def halves(cols):
    first = cols // 256 * 128
    return (0, first), (first, cols - first)


class SquareGather:
    def __init__(self, items, send_sem, recv_sem, siblings=True):
        self.items, self.send_sem, self.recv_sem, self.siblings = items, send_sem, recv_sem, siblings
        self.me, xp, yp, self.dg = square_peers()
        self.ways = ((xp, yp), (yp, xp))
        self.core = lax.axis_index("dp")

    def place(self, i, chip):
        return self.items[i][1](chip)

    def copy(self, i, k):
        first, second = self.ways[i % 2]
        own = self.items[i][0]
        src, dst, axis, peer = {
            0: (own, self.me, "wide", first),
            1: (own, self.me, "wide", second),
            2: (own, self.me, "dp", 1 - self.core),
            3: (None, first, "wide", second),
            4: (None, first, "dp", 1 - self.core),
            5: (None, second, "dp", 1 - self.core),
            6: (None, self.dg, "dp", 1 - self.core),
        }[k]
        dst = self.place(i, dst)
        return remote(dst if src is None else src, dst, self.send_sem.at[i, k], self.recv_sem.at[i, k], axis, peer)

    def start(self):
        for k in range(3 if self.siblings else 2):
            for i in range(len(self.items)):
                self.copy(i, k).start()
        for i in range(len(self.items)):
            self.place(i, self.me)[...] = self.items[i][0][...]

    def relay(self, i):
        self.copy(i, 0).wait_recv()
        self.copy(i, 3).start()
        if self.siblings:
            self.copy(i, 4).start()
            self.copy(i, 1).wait_recv()
            self.copy(i, 5).start()

    def finish(self):
        if self.siblings:
            for i in range(len(self.items)):
                self.copy(i, 3).wait_recv()
                self.copy(i, 6).start()
        for i in range(len(self.items)):
            for k in (2, 4, 5, 6) if self.siblings else (1, 3):
                self.copy(i, k).wait_recv()
            for k in range(7) if self.siblings else (0, 1, 3):
                self.copy(i, k).wait_send()


def gather_items(own_refs, whole_refs):
    core = lax.axis_index("dp")
    return [
        (own.at[:, pl.ds(*span)], lambda chip, span=span, whole=whole: whole.at[chip * 2 + core, :, pl.ds(*span)])
        for own, whole in zip(own_refs, whole_refs)
        for span in halves(own.shape[1])
    ]


class LineGather:
    def __init__(self, own_ref, place, send_sem, recv_sem, core_send=None, core_recv=None):
        self.own_ref, self.place, self.send_sem, self.recv_sem = own_ref, place, send_sem, recv_sem
        self.core_send, self.core_recv = core_send, core_recv
        self.core = lax.axis_index("dp")
        self.n, self.count, self.has_down, self.has_up = line_sides()

    def copy(self, block, way, src=None):
        place = self.place(block)
        return remote(
            place if src is None else src,
            place,
            self.send_sem.at[way, block],
            self.recv_sem.at[block],
            "narrow",
            self.n + 1 - 2 * way,
        )

    def share(self, block, src=None):
        place = self.place(block)
        return remote(
            place if src is None else src, place, self.core_send.at[block], self.core_recv.at[block], "dp", 1 - self.core
        )

    def start(self):
        @pl.when(self.has_up)
        def _():
            self.copy(self.n, 0, self.own_ref).start()

        @pl.when(self.has_down)
        def _():
            self.copy(self.n, 1, self.own_ref).start()

        if self.core_send is not None:
            self.share(self.n, self.own_ref).start()
        self.place(self.n)[...] = self.own_ref[...]

    def step(self, step):
        below, above = self.n - step, self.n + step

        @pl.when(below >= 0)
        def _():
            self.copy(below, 0).wait_recv()

            @pl.when(self.has_up)
            def _():
                self.copy(below, 0).start()

            if self.core_send is not None:
                self.share(below).start()

        @pl.when(above < self.count)
        def _():
            self.copy(above, 1).wait_recv()

            @pl.when(self.has_down)
            def _():
                self.copy(above, 1).start()

            if self.core_send is not None:
                self.share(above).start()

    def finish(self):
        for step in range(self.count):
            below, above = self.n - step, self.n + step

            @pl.when((below >= 0) & self.has_up)
            def _():
                self.copy(below, 0).wait_send()

            @pl.when((above < self.count) & self.has_down)
            def _():
                self.copy(above, 1).wait_send()

        if self.core_send is not None:
            for block in range(self.count):
                self.share(block).wait()


def lane_block(ref, index):
    return ref.at[:, pl.ds(pl.multiple_of(index * 128, 128), 128)]


def own_rows(half):
    return pl.ds(pl.multiple_of(lax.axis_index("dp") * half, 8), half)


def front_kernel(
    x_ref, dy_ref, gain_ref, shift_ref, vec_ref, bias_ref, wo_ref, wq_ref, wf_ref,
    norm_ref, stat_ref, xt_ref, dyt_ref, vecs_ref, biases_ref, wos_ref, wqs_ref, wfs_ref,
    dy_half, sums, all_sums, wo_own, wo_parts, wo_row, wq_own, wf_own,
    send_sem, recv_sem, near_send, near_recv, line_send, line_recv, core_send, core_recv, square_send, square_recv,
    early_send, early_recv,
):
    feats, tokens = x_ref.shape
    wide = 4
    block = tokens // wide
    me, xp, yp, dg = square_peers()
    peers = (xp, yp, dg)
    n, count = lax.axis_index("narrow"), lax.axis_size("narrow")
    core = lax.axis_index("dp")
    others = [lax.rem(n + k, count) for k in range(1, count)]
    part = wo_ref.shape[1]
    half = feats // 2
    wo_own[...] = wo_ref[own_rows(half), :].astype(BF)
    for k in range(3):
        wq_own[:, k * part : (k + 1) * part] = wq_ref[k, own_rows(half), :].astype(BF)
    greet(
        [("wide", peer) for peer in peers] + [("narrow", peer) for peer in others] + [("dp", 1 - core)]
    )
    copies = []

    def send(src, dst, sems, k, j, axis, peer):
        copy = remote(src, dst, sems[0].at[k, j], sems[1].at[k, j], axis, peer)
        copy.start()
        copies.append(copy)

    near, across = (near_send, near_recv), (send_sem, recv_sem)
    for j, peer in enumerate(others):
        send(wo_own, wo_parts.at[n], near, 0, j, "narrow", peer)
        send(bias_ref, biases_ref.at[n], near, 1, j, "narrow", peer)
    line = LineGather(wq_own, lambda b: wqs_ref.at[b, core], line_send, line_recv, core_send, core_recv)
    line.start()
    x = x_ref[...]
    sums[...] = jnp.zeros_like(sums)
    stat_ref[...] = jnp.zeros_like(stat_ref)
    sums[0:1, :] = jnp.sum(x, axis=0, keepdims=True)
    sums[1:2, :] = jnp.sum(x * x, axis=0, keepdims=True)
    for j, peer in enumerate(peers):
        send(sums, all_sums.at[me], across, 0, j, "wide", peer)
        send(vec_ref, vecs_ref.at[me], across, 1, j, "wide", peer)
    dy_half[...] = dy_ref[...].astype(BF)
    wo_parts[n] = wo_own[...]
    biases_ref[n] = bias_ref[...]
    vecs_ref[me] = vec_ref[...]
    mine = pl.ds(pl.multiple_of(me * feats, 16), feats)
    for k, (src, dst) in enumerate(((dy_half, dyt_ref), (x_ref, xt_ref))):
        for j, peer in enumerate(peers):
            send(lane_block(src, peer), dst.at[mine, :], across, 2 + k, j, "wide", peer)
        dst[mine, :] = lane_block(src, me)[...]
    wf_own[...] = wf_ref[own_rows(half), : wf_own.shape[1]].astype(BF)
    early = SquareGather(gather_items((wf_own,), (wfs_ref,)), early_send, early_recv)
    early.start()
    for copy in copies[: 2 * (count - 1)]:
        copy.wait()
    for k in range(count):
        wo_row[:, k * part : (k + 1) * part] = wo_parts[k]
    gather = SquareGather(gather_items((wo_row,), (wos_ref,)), square_send, square_recv)
    gather.start()
    rest = copies[2 * (count - 1) :]
    for copy in rest[:6]:
        copy.wait()
    total = sums[...]
    for peer in peers:
        total = total + all_sums[peer]
    width = feats * wide
    mean = total[0:1, :] / width
    inv = lax.rsqrt(total[1:2, :] / width - mean * mean + EPS)
    stat_ref[0:1, :] = mean
    stat_ref[1:2, :] = inv
    line.step(1)
    norm_ref[...] = ((x_ref[...] - mean) * inv * gain_ref[...] + shift_ref[...]).astype(BF)
    early.relay(0)
    early.relay(1)
    line.step(2)
    gather.relay(0)
    gather.relay(1)
    for step in range(3, count):
        line.step(step)
    for copy in rest[6:]:
        copy.wait()
    early.finish()
    gather.finish()
    line.finish()


def front_stage(x, dy, gain, shift, vec, bias, wo, wq, wf):
    feats, tokens = x.shape
    count = lax.axis_size("narrow")
    half, part = feats // 2, wo.shape[1]
    width = part * count
    ahead = halves(wf.shape[1])[0][1]
    return pl.pallas_call(
        front_kernel,
        out_shape=(
            shape_of((feats, tokens), BF),
            shape_of((8, tokens), F32),
            shape_of((4 * feats, tokens // 4), F32),
            shape_of((4 * feats, tokens // 4), BF),
            shape_of((4,) + vec.shape, F32),
            shape_of((count,) + bias.shape, F32),
            shape_of((8, half, width), BF),
            shape_of((count, 2, half, 3 * part), BF),
            shape_of((8, half, ahead), BF),
        ),
        in_specs=in_vmem(9),
        out_specs=tuple(in_vmem(9)),
        scratch_shapes=[
            pltpu.VMEM((feats, tokens), BF),
            pltpu.VMEM((8, tokens), F32),
            pltpu.VMEM((4, 8, tokens), F32),
            pltpu.VMEM((half, part), BF),
            pltpu.VMEM((count, half, part), BF),
            pltpu.VMEM((half, width), BF),
            pltpu.VMEM((half, 3 * part), BF),
            pltpu.VMEM((half, ahead), BF),
            pltpu.SemaphoreType.DMA((4, 3)),
            pltpu.SemaphoreType.DMA((4, 3)),
            pltpu.SemaphoreType.DMA((2, count - 1)),
            pltpu.SemaphoreType.DMA((2, count - 1)),
            pltpu.SemaphoreType.DMA((2, count)),
            pltpu.SemaphoreType.DMA((count,)),
            pltpu.SemaphoreType.DMA((count,)),
            pltpu.SemaphoreType.DMA((count,)),
            pltpu.SemaphoreType.DMA((2, 7)),
            pltpu.SemaphoreType.DMA((2, 7)),
            pltpu.SemaphoreType.DMA((2, 7)),
            pltpu.SemaphoreType.DMA((2, 7)),
        ],
        compiler_params=params(1),
        cost_estimate=pl.CostEstimate(flops=10**10, bytes_accessed=60 * 10**6, transcendentals=0),
        name="front_stage",
    )(x, dy, gain, shift, vec, bias, wo, wq, wf)


def qkv_kernel(
    norm_ref, w_ref, bias_ref, dy_ref, out_ref, dys_ref,
    acc, first_out, first_in, second_out, second_in, send_sem, recv_sem, line_send, line_recv,
):
    pieces, feats, cols = w_ref.shape
    tokens = norm_ref.shape[0]
    block = tokens // 4
    me, xp, yp, dg = square_peers()
    greet((("wide", xp), ("wide", yp)), line_sides())
    line = LineGather(dy_ref, lambda b: lane_block(dys_ref, b), line_send, line_recv)
    line.start()

    def rows(index):
        return pl.ds(pl.multiple_of(index * block, block), block)

    def ways(p):
        turn = lax.rem(p, 2)
        return xp * (1 - turn) + yp * turn, yp * (1 - turn) + xp * turn

    def first_copy(p):
        return remote(first_out.at[p], first_in.at[p], send_sem.at[0, p], recv_sem.at[0, p], "wide", ways(p)[0])

    def second_copy(p):
        return remote(second_out.at[p], second_in.at[p], send_sem.at[1, p], recv_sem.at[1, p], "wide", ways(p)[1])

    def issue(p, carry):
        acc[p] = dot(norm_ref[...], w_ref[p], 1, 0)
        first_out[p, 0] = acc[p, rows(ways(p)[0]), :].astype(BF)
        first_out[p, 1] = acc[p, rows(dg), :].astype(BF)
        first_copy(p).start()
        return carry

    lax.fori_loop(0, pieces, issue, 0)
    line.step(1)

    def middle(p, carry):
        first_copy(p).wait()
        second_out[p] = (acc[p, rows(ways(p)[1]), :] + first_in[p, 1].astype(F32)).astype(BF)
        second_copy(p).start()
        return carry

    lax.fori_loop(0, pieces // 2, middle, 0)
    line.step(2)
    lax.fori_loop(pieces // 2, pieces, middle, 0)
    for step in range(3, line.count):
        line.step(step)

    def last(p, carry):
        second_copy(p).wait()
        total = acc[p, rows(me), :] + first_in[p, 0].astype(F32) + second_in[p].astype(F32)
        out_ref[p] = (total + bias_ref[p]).astype(BF)
        return carry

    lax.fori_loop(0, pieces, last, 0)
    line.finish()


def qkv_stage(norm, w, bias, dy):
    count = lax.axis_size("narrow")
    pieces, feats, cols = w.shape
    tokens = norm.shape[0]
    block = tokens // 4
    return pl.pallas_call(
        qkv_kernel,
        out_shape=(shape_of((pieces, block, cols), BF), shape_of((dy.shape[0], count * dy.shape[1]), BF)),
        in_specs=in_vmem(4),
        out_specs=tuple(in_vmem(2)),
        scratch_shapes=[
            pltpu.VMEM((pieces, tokens, cols), F32),
            pltpu.VMEM((pieces, 2, block, cols), BF),
            pltpu.VMEM((pieces, 2, block, cols), BF),
            pltpu.VMEM((pieces, block, cols), BF),
            pltpu.VMEM((pieces, block, cols), BF),
            pltpu.SemaphoreType.DMA((2, pieces)),
            pltpu.SemaphoreType.DMA((2, pieces)),
            pltpu.SemaphoreType.DMA((2, count)),
            pltpu.SemaphoreType.DMA((count,)),
        ],
        compiler_params=params(2),
        cost_estimate=pl.CostEstimate(flops=3 * 10**10, bytes_accessed=10**8, transcendentals=0),
        name="qkv_stage",
    )(norm, w, bias, dy)


def pair_kernel(
    own_ref, ahead_ref, wf_ref, wp_ref, all_ref, wfs_ref, wps_ref,
    wf_own, wp_own, send_sem, recv_sem, line_send, line_recv, local_sem,
):
    me, xp, yp, dg = square_peers()
    half, ahead = wp_own.shape[0], ahead_ref.shape[2]
    wf_own[...] = wf_ref[own_rows(half), ahead:].astype(BF)
    wp_own[...] = wp_ref[own_rows(half), :].astype(BF)
    greet((("wide", xp), ("wide", yp), ("dp", 1 - lax.axis_index("dp"))), line_sides())
    line = LineGather(own_ref, lambda b: lane_block(all_ref, b), line_send, line_recv)
    line.start()
    rest = wfs_ref.at[:, :, pl.ds(ahead, wf_own.shape[1])]
    gather = SquareGather(gather_items((wf_own, wp_own), (rest, wps_ref)), send_sem, recv_sem)
    gather.start()
    move = pltpu.make_async_copy(ahead_ref, wfs_ref.at[:, :, pl.ds(0, ahead)], local_sem)
    move.start()
    line.step(1)
    gather.relay(0)
    gather.relay(1)
    line.step(2)
    gather.relay(2)
    gather.relay(3)
    for step in range(3, line.count):
        line.step(step)
    gather.finish()
    line.finish()
    move.wait()


def pair_stage(own, ahead, wf, wp):
    count = lax.axis_size("narrow")
    rows, cols = wf.shape[0] // 2, wf.shape[1]
    return pl.pallas_call(
        pair_kernel,
        out_shape=(
            shape_of((own.shape[0], count * own.shape[1]), own.dtype),
            shape_of((8, rows, cols), BF),
            shape_of((8, rows, cols), BF),
        ),
        in_specs=in_vmem(4),
        out_specs=tuple(in_vmem(3)),
        scratch_shapes=[
            pltpu.VMEM((rows, cols - ahead.shape[2]), BF),
            pltpu.VMEM((rows, cols), BF),
            pltpu.SemaphoreType.DMA((4, 7)),
            pltpu.SemaphoreType.DMA((4, 7)),
            pltpu.SemaphoreType.DMA((2, count)),
            pltpu.SemaphoreType.DMA((count,)),
            pltpu.SemaphoreType.DMA,
        ],
        compiler_params=params(7),
        cost_estimate=pl.CostEstimate(flops=2 * 10**10, bytes_accessed=7 * 10**7, transcendentals=0),
        name="pair_stage",
    )(own, ahead, wf, wp)


class SquareSum:
    def __init__(self, part_ref, bufs, sems):
        self.part_ref = part_ref
        self.core_in, self.half, self.first_out, self.first_in, self.second_out, self.second_in = bufs
        self.core_send, self.core_recv, self.send_sem, self.recv_sem = sems
        self.me, xp, yp, self.dg = square_peers()
        self.ways = ((xp, yp), (yp, xp))
        self.core = lax.axis_index("dp")
        self.spans = halves(part_ref.shape[2])

    def core_copy(self, chip):
        return remote(
            self.part_ref.at[chip * 2 + 1 - self.core],
            self.core_in.at[chip],
            self.core_send.at[chip],
            self.core_recv.at[chip],
            "dp",
            1 - self.core,
        )

    def first_copy(self, i, k):
        cols = pl.ds(*self.spans[i])
        return remote(
            self.first_out.at[k, :, cols],
            self.first_in.at[k, :, cols],
            self.send_sem.at[i, k],
            self.recv_sem.at[i, k],
            "wide",
            self.ways[i][0],
        )

    def second_copy(self, i):
        cols = pl.ds(*self.spans[i])
        return remote(
            self.second_out.at[:, cols],
            self.second_in.at[:, cols],
            self.send_sem.at[i, 2],
            self.recv_sem.at[i, 2],
            "wide",
            self.ways[i][1],
        )

    def start(self):
        for chip in range(4):
            self.core_copy(chip).start()

    def issue(self):
        for chip in range(4):
            self.core_copy(chip).wait()
            total = self.part_ref[chip * 2 + self.core].astype(F32) + self.core_in[chip].astype(F32)
            self.half[chip] = total.astype(BF)
        for i, (at, size) in enumerate(self.spans):
            for k, chip in enumerate((self.ways[i][0], self.dg)):
                self.first_out[k, :, at : at + size] = self.half[chip, :, at : at + size]
                self.first_copy(i, k).start()

    def middle(self):
        for i, (at, size) in enumerate(self.spans):
            self.first_copy(i, 1).wait()
            total = self.half[self.ways[i][1], :, at : at + size].astype(F32)
            total = total + self.first_in[1, :, at : at + size].astype(F32)
            self.second_out[:, at : at + size] = total.astype(BF)
            self.second_copy(i).start()

    def finish(self, write):
        for i, (at, size) in enumerate(self.spans):
            self.first_copy(i, 0).wait()
            self.second_copy(i).wait()
            total = self.half[self.me, :, at : at + size].astype(F32)
            total = total + self.first_in[0, :, at : at + size].astype(F32)
            write(at, size, total + self.second_in[:, at : at + size].astype(F32))


def square_sum_scratch(rows, cols):
    return [
        pltpu.VMEM((4, rows, cols), BF),
        pltpu.VMEM((4, rows, cols), BF),
        pltpu.VMEM((2, rows, cols), BF),
        pltpu.VMEM((2, rows, cols), BF),
        pltpu.VMEM((rows, cols), BF),
        pltpu.VMEM((rows, cols), BF),
        pltpu.SemaphoreType.DMA((4,)),
        pltpu.SemaphoreType.DMA((4,)),
        pltpu.SemaphoreType.DMA((2, 3)),
        pltpu.SemaphoreType.DMA((2, 3)),
    ]


def ffn_back_kernel(
    part_ref, out_part_ref, cot_ref, hidden_ref, norm_ref, pre_ref, att_ref,
    sum_ref, out_sum_ref, wp_ref, wf_ref, atts_ref,
    wp_part, wf_part, leave, arrive, line_send, line_recv, share_send, share_recv, att_send, att_recv, *square,
):
    me, xp, yp, dg = square_peers()
    n, count, has_down, has_up = line_sides()
    core = lax.axis_index("dp")
    greet((("wide", xp), ("wide", yp), ("dp", 1 - core)), line_sides())
    rows = wp_part.shape[1]

    lines = ((part_ref, sum_ref), (out_part_ref, out_sum_ref))

    def line_copy(k, way, b):
        return remote(
            leave.at[k, way, b],
            arrive.at[k, way, b],
            line_send.at[k, way, b],
            line_recv.at[k, way, b],
            "narrow",
            n + 1 - 2 * way,
        )

    def turn(k, way, b, sends, joins):
        own = lines[k][0]

        @pl.when(sends & joins)
        def _():
            line_copy(k, way, b).wait_recv()
            total = own[:, b * 128 : (b + 1) * 128].astype(F32) + arrive[k, way, b].astype(F32)
            leave[k, way, b] = total.astype(BF)
            line_copy(k, way, b).start()

        @pl.when(sends & jnp.logical_not(joins))
        def _():
            leave[k, way, b] = own[:, b * 128 : (b + 1) * 128]
            line_copy(k, way, b).start()

    def turns(k, slot):
        for step in range(count - 1):
            hop = slot - step
            turn(k, 0, count - 1 - step, (n == hop) & (n < count - 1 - step), has_down)
            turn(k, 1, step, (count - 1 - n == hop) & (n > step), has_up)

    sums = [
        SquareSum(ref, square[10 * k : 10 * k + 6], square[10 * k + 6 : 10 * k + 10])
        for k, ref in enumerate((wp_part, wf_part))
    ]

    def products(total, left, right):
        def step(i, carry):
            chip = lax.rem(i, 4)
            index = chip * 2 + core + (1 - 2 * core) * (1 - i // 4)
            at = pl.ds(pl.multiple_of(index * rows, 8), rows)
            total.part_ref[index] = dot(left[at, :], right[...], 1, 1).astype(BF)

            @pl.when(i < 4)
            def _():
                total.core_copy(chip).start()

            return carry

        lax.fori_loop(0, 8, step, 0)

    block = att_ref.shape[1]
    gather = SquareGather(
        [
            (
                att_ref.at[p],
                lambda chip, p=p: atts_ref.at[p, pl.ds(pl.multiple_of(chip * block, block), block), :],
            )
            for p in range(att_ref.shape[0])
        ],
        att_send,
        att_recv,
        siblings=False,
    )
    slots = 2 * count - 3
    turns(0, 0)
    turns(1, 0)
    gather.start()
    products(sums[0], cot_ref, hidden_ref)
    sums[0].issue()
    turns(0, 1)
    products(sums[1], norm_ref, pre_ref)
    sums[1].issue()
    turns(1, 1)
    for p in range(att_ref.shape[0]):
        gather.relay(p)
    turns(0, 2)
    sums[0].middle()
    turns(1, 2)
    sums[1].middle()
    for slot in range(3, slots):
        turns(0, slot)
        turns(1, slot)
    for k, (own, out) in enumerate(lines):
        out[...] = lane_block(own, n)[...].astype(F32)
        for way, joins in ((0, has_down), (1, has_up)):

            @pl.when(joins)
            def _():
                line_copy(k, way, n).wait_recv()
                out[...] += arrive[k, way, n].astype(F32)

    shares = []
    for k, out in enumerate((wp_ref, wf_ref)):

        def write(at, size, value):
            out[core, :, at : at + size] = value.astype(BF)

        sums[k].finish(write)
        copy = remote(out.at[core], out.at[core], share_send.at[k], share_recv.at[k], "dp", 1 - core)
        copy.start()
        shares.append(copy)
    for k in range(2):
        for step in range(count - 1):

            @pl.when(n < count - 1 - step)
            def _():
                line_copy(k, 0, count - 1 - step).wait_send()

            @pl.when(n > step)
            def _():
                line_copy(k, 1, step).wait_send()

    gather.finish()
    for copy in shares:
        copy.wait()


def ffn_back_stage(part, out_part, cot, hidden, norm, pre, attended):
    count = lax.axis_size("narrow")
    width, tokens = part.shape
    hid = hidden.shape[0]
    rows = width // 8
    return pl.pallas_call(
        ffn_back_kernel,
        out_shape=(
            shape_of((width, tokens // count), F32),
            shape_of((width, tokens // count), F32),
            shape_of((2, rows, hid), BF),
            shape_of((2, rows, hid), BF),
            shape_of((attended.shape[0], 4 * attended.shape[1], attended.shape[2]), BF),
        ),
        in_specs=in_vmem(7),
        out_specs=tuple(in_vmem(5)),
        scratch_shapes=[
            pltpu.VMEM((8, rows, hid), BF),
            pltpu.VMEM((8, rows, hid), BF),
            pltpu.VMEM((2, 2, count, width, tokens // count), BF),
            pltpu.VMEM((2, 2, count, width, tokens // count), BF),
            pltpu.SemaphoreType.DMA((2, 2, count)),
            pltpu.SemaphoreType.DMA((2, 2, count)),
            pltpu.SemaphoreType.DMA((2,)),
            pltpu.SemaphoreType.DMA((2,)),
            pltpu.SemaphoreType.DMA((attended.shape[0], 7)),
            pltpu.SemaphoreType.DMA((attended.shape[0], 7)),
        ]
        + square_sum_scratch(rows, hid)
        + square_sum_scratch(rows, hid),
        compiler_params=params(5),
        cost_estimate=pl.CostEstimate(flops=4 * 10**10, bytes_accessed=10**8, transcendentals=0),
        name="ffn_back_stage",
    )(part, out_part, cot, hidden, norm, pre, attended)


TOKEN_TERMS = 5


def back_kernel(
    cot_ref, norm_ref, w_ref, att_ref, resid_ref, x_ref, dy_ref, stat_ref, gain_ref, terms_ref,
    out_ref, wq_out, wo_out, terms_out, feat_out,
    grad_ref, cots, full, other, core_in, leave, arrive,
    resid_in, columns, sums, all_sums, terms_in, terms_mid, line_terms, feat, line_feat, terms_two, terms_last,
    feat_two, feat_last,
    send_sem, recv_sem, core_send, core_recv, line_send, line_recv, share_send, share_recv,
    around_send, around_recv, along_send, along_recv,
):
    pieces, block, cols = cot_ref.shape
    feats, tokens = norm_ref.shape
    me, xp, yp, dg = square_peers()
    peers = (xp, yp, dg)
    n, count, has_down, has_up = line_sides()
    core = lax.axis_index("dp")
    others = [lax.rem(n + k, count) for k in range(1, count)]
    greet(
        [("wide", peer) for peer in peers] + [("narrow", peer) for peer in others] + [("dp", 1 - core)]
    )
    spans = halves(cols)
    ways = ((xp, yp), (yp, xp))
    rows_half = core_in.shape[1]

    def order(i):
        odd = lax.rem(i, 2)
        return (1 - odd) * (i // 2) + odd * (pieces - 1 - i // 2)

    def rows(index):
        return pl.ds(pl.multiple_of(index * block, block), block)

    def spread(i, h, k):
        p = order(i)
        span = pl.ds(*spans[h])
        first, second = ways[h]
        place = cots.at[p, rows(first if k == 2 else me), span]
        src = place if k == 2 else cot_ref.at[p, :, span]
        return remote(
            src, place, send_sem.at[h, k, p], recv_sem.at[h, k, p], "wide", first if k == 0 else second
        )

    def own(i):
        for h in range(2):
            for k in range(2):
                spread(i, h, k).start()
        p = order(i)
        cots[p, rows(me), :] = cot_ref[p]

    def around(k, src, dst, start=True):
        copies = []
        for j, peer in enumerate(peers):
            copy = remote(src(peer), dst, around_send.at[k, j], around_recv.at[k, j], "wide", peer)
            if start:
                copy.start()
            copies.append(copy)
        return copies

    def resid_moves(start):
        return around(
            1, lambda peer: resid_ref.at[pl.ds(pl.multiple_of(peer * feats, 16), feats), :], resid_in.at[me], start
        )

    def along(k, src, dst):
        copies = []
        for j, peer in enumerate(others):
            copy = remote(src, dst, along_send.at[k, j], along_recv.at[k, j], "narrow", peer)
            copy.start()
            copies.append(copy)
        return copies

    def core_copy(p):
        return remote(other.at[p], core_in.at[p], core_send.at[p], core_recv.at[p], "dp", 1 - core)

    whole = halves(full.shape[2])

    def line_copy(way, p, h):
        span = pl.ds(*whole[h])
        return remote(
            leave.at[p, :, span],
            arrive.at[way, p, :, span],
            line_send.at[p, h],
            line_recv.at[way, p, h],
            "narrow",
            n + 1 - 2 * way,
        )

    mine_rows = own_rows(rows_half)
    sibling_rows = pl.ds(pl.multiple_of((1 - core) * rows_half, 8), rows_half)
    terms_moves = around(0, lambda peer: terms_ref, terms_in.at[me])
    own(0)
    resid_moves(True)
    resid_in[me] = resid_ref[pl.ds(pl.multiple_of(me * feats, 16), feats), :]
    grad_ref[...] = jnp.zeros_like(grad_ref)
    for copy in terms_moves:
        copy.wait()
    total = terms_ref[...]
    for peer in peers:
        total = total + terms_in[peer]
    terms_mid[...] = total
    terms_moves = along(0, terms_mid, line_terms.at[n])

    def pass_on(way, p, joins):
        for h, (at, size) in enumerate(whole):

            @pl.when(joins)
            def _():
                line_copy(way, p, h).wait_recv()
                mine = full[p, mine_rows, at : at + size]
                leave[p, :, at : at + size] = (mine + arrive[way, p, :, at : at + size].astype(F32)).astype(BF)

            @pl.when(jnp.logical_not(joins))
            def _():
                leave[p, :, at : at + size] = full[p, mine_rows, at : at + size].astype(BF)

            line_copy(way, p, h).start()

    def body(i, carry):
        @pl.when(i < pieces)
        def _():
            for h in range(2):
                spread(i, h, 0).wait_recv()
                spread(i, h, 2).start()

        @pl.when(i == 0)
        def _():
            own(1)

        @pl.when(i + 2 < pieces)
        def _():
            own(i + 2)

        @pl.when(i == 1)
        def _():
            for copy in resid_moves(False):
                copy.wait()

        @pl.when((i >= 1) & (i <= pieces))
        def _():
            p = order(i - 1)
            for h in range(2):
                spread(i - 1, h, 1).wait_recv()
                spread(i - 1, h, 2).wait_recv()
            full[p, :, :cols] = dot(norm_ref[...], cots[p], 1, 0)
            total = dot(resid_in[0], att_ref[p, :block, :], 1, 0)
            for chip in range(1, 4):
                total = total + dot(resid_in[chip], att_ref[p, chip * block : (chip + 1) * block, :], 1, 0)
            full[p, :, cols:] = total
            other[p] = full[p, sibling_rows, :].astype(BF)
            core_copy(p).start()
            grad_ref[...] += dot(w_ref[p], cots[p], 1, 1)
            core_copy(p).wait()
            full[p, mine_rows, :] = full[p, mine_rows, :] + core_in[p].astype(F32)

        @pl.when(i == pieces)
        def _():
            scaled = grad_ref[...] * gain_ref[...]
            normed = (x_ref[...] - stat_ref[0:1, :]) * stat_ref[1:2, :]
            sums[0:1, :] = jnp.sum(scaled, axis=0, keepdims=True)
            sums[1:2, :] = jnp.sum(scaled * normed, axis=0, keepdims=True)
            around(2, lambda peer: sums, all_sums.at[me])

        for hop in range(count - 1):
            turn = i - 1 - hop
            p = order(turn)
            here = (turn >= 0) & (turn < pieces)

            @pl.when(here & (n < p) & (n == hop))
            def _():
                pass_on(0, p, has_down)

            @pl.when(here & (n > p) & (count - 1 - n == hop))
            def _():
                pass_on(1, p, has_up)

        return carry

    sums[...] = jnp.zeros_like(sums)
    lax.fori_loop(0, pieces + count - 1, body, 0)
    inv = stat_ref[1:2, :]
    normed = (x_ref[...] - stat_ref[0:1, :]) * inv
    grad = grad_ref[...]
    scaled = grad * gain_ref[...]
    columns[...] = jnp.zeros_like(columns)
    columns[:feats, 0:1] = jnp.sum(grad * normed, axis=1, keepdims=True)
    columns[:feats, 1:2] = jnp.sum(grad, axis=1, keepdims=True)
    columns[:feats, 2:3] = jnp.sum(dy_ref[...], axis=1, keepdims=True)
    feat[...] = jnp.transpose(columns[...])[:8, :]
    feat_moves = along(1, feat, line_feat.at[n])
    for copy in around(2, lambda peer: sums, all_sums.at[me], False):
        copy.wait()
    total = sums[...]
    for peer in peers:
        total = total + all_sums[peer]
    width = feats * 4
    back = inv * (scaled - total[0:1, :] / width - normed * (total[1:2, :] / width))
    for k in range(4):
        at = slice(k * block, (k + 1) * block)
        out_ref[:, at] = resid_in[k].astype(F32) + back[:, at]

    for copy in terms_moves + feat_moves:
        copy.wait()
    total, feat_total = terms_mid[...], feat[...]
    shared = lax.broadcasted_iota(jnp.int32, total.shape, 0) < TOKEN_TERMS
    for peer in others:
        total = total + jnp.where(shared, line_terms[peer], 0.0)
        feat_total = feat_total + line_feat[peer]
    terms_two[...] = total
    feat_two[...] = feat_total
    shares = []

    def share(k, src, dst):
        copy = remote(src, dst, share_send.at[k], share_recv.at[k], "dp", 1 - core)
        copy.start()
        shares.append(copy)

    share(2, terms_two, terms_last)
    share(3, feat_two, feat_last)
    for way, joins in ((0, has_down), (1, has_up)):

        @pl.when(joins)
        def _():
            for h in range(2):
                line_copy(way, n, h).wait_recv()
            full[n, mine_rows, :] += arrive[way, n].astype(F32)

    part = wo_out.shape[2]
    wo_out[core] = full[n, mine_rows, cols:]
    share(1, wo_out.at[core], wo_out.at[core])
    for k in range(3):
        wq_out[k, core] = full[n, mine_rows, k * part : (k + 1) * part]
        share(4 + k, wq_out.at[k, core], wq_out.at[k, core])

    def drain(i, carry):
        for h in range(2):
            for k in range(3):
                spread(i, h, k).wait_send()
        p = order(i)

        @pl.when(n < p)
        def _():
            line_copy(0, p, 0).wait_send()
            line_copy(0, p, 1).wait_send()

        @pl.when(n > p)
        def _():
            line_copy(1, p, 0).wait_send()
            line_copy(1, p, 1).wait_send()

        return carry

    lax.fori_loop(0, pieces, drain, 0)
    for copy in shares:
        copy.wait()
    terms_out[...] = total + terms_last[...]
    feat_out[...] = feat_total + feat_last[...]


def back_stage(cot, norm, w, attended, resid, x, dy, stats, gain, terms):
    pieces, block, cols = cot.shape
    count = lax.axis_size("narrow")
    feats, tokens = norm.shape
    half, part = feats // 2, cols // 3
    both = cols + part
    long = -(-feats // 128) * 128
    return pl.pallas_call(
        back_kernel,
        out_shape=(
            shape_of((feats, tokens), F32),
            shape_of((3, 2, half, part), F32),
            shape_of((2, half, part), F32),
            shape_of(terms.shape, F32),
            shape_of((8, long), F32),
        ),
        in_specs=in_vmem(10),
        out_specs=tuple(in_vmem(5)),
        scratch_shapes=[
            pltpu.VMEM((feats, tokens), F32),
            pltpu.VMEM((pieces, tokens, cols), BF),
            pltpu.VMEM((pieces, feats, both), F32),
            pltpu.VMEM((pieces, half, both), BF),
            pltpu.VMEM((pieces, half, both), BF),
            pltpu.VMEM((pieces, half, both), BF),
            pltpu.VMEM((2, pieces, half, both), BF),
            pltpu.VMEM((4, feats, block), BF),
            pltpu.VMEM((long, 128), F32),
            pltpu.VMEM((8, tokens), F32),
            pltpu.VMEM((4, 8, tokens), F32),
            pltpu.VMEM((4,) + terms.shape, F32),
            pltpu.VMEM(terms.shape, F32),
            pltpu.VMEM((count,) + terms.shape, F32),
            pltpu.VMEM((8, long), F32),
            pltpu.VMEM((count, 8, long), F32),
            pltpu.VMEM(terms.shape, F32),
            pltpu.VMEM(terms.shape, F32),
            pltpu.VMEM((8, long), F32),
            pltpu.VMEM((8, long), F32),
            pltpu.SemaphoreType.DMA((2, 3, pieces)),
            pltpu.SemaphoreType.DMA((2, 3, pieces)),
            pltpu.SemaphoreType.DMA((pieces,)),
            pltpu.SemaphoreType.DMA((pieces,)),
            pltpu.SemaphoreType.DMA((pieces, 2)),
            pltpu.SemaphoreType.DMA((2, pieces, 2)),
            pltpu.SemaphoreType.DMA((7,)),
            pltpu.SemaphoreType.DMA((7,)),
            pltpu.SemaphoreType.DMA((3, 3)),
            pltpu.SemaphoreType.DMA((3, 3)),
            pltpu.SemaphoreType.DMA((2, count - 1)),
            pltpu.SemaphoreType.DMA((2, count - 1)),
        ],
        compiler_params=params(3),
        cost_estimate=pl.CostEstimate(flops=4 * 10**10, bytes_accessed=10**8, transcendentals=0),
        name="back_stage",
    )(cot, norm, w, attended, resid, x, dy, stats, gain, terms)


def as_rows(rows):
    return jnp.concatenate([jnp.stack(rows), jnp.zeros((8 - len(rows), rows[0].shape[0]), F32)])


def own_half(values, axis):
    half = values.shape[axis] // lax.axis_size("dp")
    return lax.dynamic_slice_in_dim(values, lax.axis_index("dp") * half, half, axis)


def local(
    block_input,
    block_cotangent,
    seq_start,
    ln1_gain,
    ln1_shift,
    w_qkv,
    b_qv,
    w_out,
    b_out,
    ln2_gain,
    ln2_shift,
    w_fc,
    b_fc,
    w_proj,
    b_proj,
):
    cores, wide, narrow = lax.axis_size("dp"), lax.axis_size("wide"), lax.axis_size("narrow")
    w_index, n_index = lax.axis_index("wide"), lax.axis_index("narrow")
    feats, part = w_qkv.shape[0], w_qkv.shape[2]
    width = feats * wide
    hid = w_fc.shape[1]

    perm = []
    for w in range(wide):
        for n in range(narrow):
            block = n * wide + w
            perm.append((block, w * narrow + n))
    starts = lax.ppermute(seq_start, ("wide", "narrow"), perm)[0]
    allowed = block_mask(starts)

    def three(biases):
        zeros = jnp.zeros((narrow, 1, part), F32)
        return jnp.concatenate([biases[:, None, 0], zeros, biases[:, None, 1]], axis=2)

    square = wide == 4 and cores == 2
    if square:
        norm_t, stats, x_tok, dy_tok, vecs, biases, wo_all, wq_all, wf_ahead = front_stage(
            block_input,
            block_cotangent,
            ln1_gain[:, None],
            ln1_shift[:, None],
            as_rows([b_out, ln2_gain, ln2_shift]),
            as_rows([b_qv[0], b_qv[1]]),
            w_out,
            w_qkv.transpose(1, 0, 2),
            w_fc,
        )
        wo_all = wo_all.reshape(width, width)
        wq_all = wq_all.reshape(narrow, feats, 3 * part)
        b_out_full, gain_two_full, shift_two_full = (vecs[:, i].reshape(width) for i in range(3))
        qkv_rows, cot_all = qkv_stage(norm_t.T, wq_all, three(biases), dy_tok)
    else:
        wq_half = own_half(w_qkv, 0).astype(BF).reshape(-1, 3 * part)
        wo_half, wf_half, wp_half = (own_half(w, 0).astype(BF) for w in (w_out, w_fc, w_proj))
        wq_all = lax.all_gather(wq_half, ("narrow", "dp"), axis=0, tiled=True).reshape(narrow, feats, 3 * part)
        wo_mine = lax.all_gather(wo_half, "narrow", axis=1, tiled=True)
        wo_all = lax.all_gather(wo_mine, ("wide", "dp"), axis=0, tiled=True)
        wf_all = lax.all_gather(wf_half, ("wide", "dp"), axis=0, tiled=True)
        wp_all = lax.all_gather(wp_half, ("wide", "dp"), axis=0, tiled=True)
        b_out_full, gain_two_full, shift_two_full = lax.all_gather(
            jnp.stack([b_out, ln2_gain, ln2_shift]), "wide", axis=1, tiled=True
        )
        x_tok = to_tokens(block_input)
        dy_tok = to_tokens(block_cotangent)
        normed_one, inv_one, norm_one = norm_forward(block_input.T, ln1_gain, ln1_shift)
        qkv_part = jnp.einsum("tk,nkc->tnc", norm_one, wq_all, preferred_element_type=F32)
        qkv_rows = sum_tokens(qkv_part).transpose(1, 0, 2)
        qkv_rows = (qkv_rows + three(lax.all_gather(b_qv, "narrow", axis=0))).astype(BF)
        cot_all = gather_narrow(dy_tok.astype(BF))

    heads_all = qkv_rows.reshape(narrow, -1, 3, part).transpose(1, 2, 0, 3).reshape(-1, 3, width)
    attended, log_total = attend_forward(heads_all, allowed)
    residual = x_tok + dot(wo_all, attended, 1, 1) + b_out_full[:, None]
    mean_two = jnp.mean(residual, axis=0, keepdims=True)
    inv_two = lax.rsqrt(jnp.mean(residual * residual, axis=0, keepdims=True) - mean_two * mean_two + EPS)
    normed_two = (residual - mean_two) * inv_two
    norm_two = (normed_two * gain_two_full[:, None] + shift_two_full[:, None]).astype(BF)
    if square:
        norm_two_all, wf_all, wp_all = pair_stage(norm_two, wf_ahead, w_fc, w_proj)
        wf_all, wp_all = wf_all.reshape(width, hid), wp_all.reshape(width, hid)
    else:
        norm_two_all = gather_narrow(norm_two)
    pre_act = dot(wf_all, norm_two_all, 0, 0) + b_fc[:, None]
    hidden = gelu_value(pre_act).astype(BF)
    pre_grad = dot(wp_all, cot_all, 0, 0) * gelu_slope(pre_act)
    pre_cot = pre_grad.astype(BF)
    norm_two_part = dot(wf_all, pre_cot, 1, 0)

    def reduce_wide(grad):
        return lax.psum_scatter(grad.astype(BF), ("wide", "dp"), scatter_dimension=0, tiled=True)

    def share(total):
        return lax.all_gather(total, "dp", axis=0, tiled=True).astype(F32)

    if square:
        norm_two_grad, out_sum, grad_w_proj, grad_w_fc, attended_all = ffn_back_stage(
            norm_two_part.astype(BF),
            dot(wp_all, hidden, 1, 0).astype(BF),
            cot_all,
            hidden,
            norm_two_all,
            pre_cot,
            attended.reshape(-1, narrow, part).transpose(1, 0, 2),
        )
        grad_w_fc = grad_w_fc.astype(F32).reshape(w_fc.shape)
        grad_w_proj = grad_w_proj.astype(F32).reshape(w_proj.shape)
    else:
        norm_two_grad = sum_narrow(norm_two_part)
        out_sum = sum_narrow(dot(wp_all, hidden, 1, 0))
        grad_w_proj = share(reduce_wide(dot(cot_all, hidden, 1, 1)))
        grad_w_fc = share(reduce_wide(dot(norm_two_all, pre_cot, 1, 1)))
    output = to_features((residual + out_sum).astype(BF)).astype(F32) + b_proj[:, None]

    scaled = norm_two_grad * gain_two_full[:, None]
    mean_scaled = jnp.mean(scaled, axis=0, keepdims=True)
    mean_cross = jnp.mean(scaled * normed_two, axis=0, keepdims=True)
    resid_grad = dy_tok.astype(F32) + inv_two * (scaled - mean_scaled - normed_two * mean_cross)
    resid_cot = resid_grad.astype(BF)
    attended_cot = dot(resid_cot, wo_all, 0, 0).astype(BF)

    qkv_grad = attend_backward(heads_all, allowed, log_total, attended_cot)
    qkv_cot = qkv_grad.astype(BF).reshape(-1, 3, narrow, part).transpose(2, 0, 1, 3)
    qkv_cot = qkv_cot.reshape(narrow, -1, 3 * part)
    qkv_sums = jnp.sum(qkv_grad, axis=0)
    wide_terms = as_rows(
        [
            qkv_sums[0],
            qkv_sums[2],
            jnp.sum(resid_grad, axis=1),
            jnp.sum(norm_two_grad * normed_two, axis=1),
            jnp.sum(norm_two_grad, axis=1),
        ]
    )
    fc_terms = jnp.sum(pre_grad, axis=1)
    if square:
        span = max(width, hid)
        packed = jnp.zeros((8, span), F32)
        packed = packed.at[:, :width].set(wide_terms).at[TOKEN_TERMS, :hid].set(fc_terms)
        grad_input, grad_w_qkv, grad_w_out, packed_sum, feat_sum = back_stage(
            qkv_cot,
            norm_t,
            wq_all,
            attended_all,
            resid_cot,
            block_input,
            block_cotangent,
            stats,
            ln1_gain[:, None],
            packed,
        )
        grad_w_qkv = grad_w_qkv.reshape(3, feats, part).transpose(1, 0, 2)
        grad_w_out = grad_w_out.reshape(feats, part)
        token_sum = packed_sum[:TOKEN_TERMS, :width]
        grad_b_fc = packed_sum[TOKEN_TERMS, :hid]
        gain_one, shift_one, proj_bias = (feat_sum[i, :feats] for i in range(3))
    else:
        qkv_cot_all = lax.all_gather(qkv_cot, "wide", axis=1, tiled=True)
        wq_grad = jnp.einsum("tk,ntc->nkc", norm_one, qkv_cot_all, preferred_element_type=F32).astype(BF)
        wq_grad = lax.psum_scatter(
            wq_grad.reshape(narrow * feats, 3 * part), ("narrow", "dp"), scatter_dimension=0, tiled=True
        )
        grad_w_qkv = share(wq_grad).reshape(feats, 3, part)
        wo_grad = reduce_wide(dot(resid_cot, attended, 1, 0))
        wo_grad = lax.psum_scatter(wo_grad, "narrow", scatter_dimension=1, tiled=True)
        grad_w_out = share(wo_grad)
        norm_one_grad = jnp.einsum("nkc,ntc->tk", wq_all, qkv_cot_all, preferred_element_type=F32)
        grad_input = to_features(resid_grad) + norm_backward(norm_one_grad, normed_one, inv_one, ln1_gain).T
        feature_terms = jnp.stack(
            [
                jnp.sum(norm_one_grad * normed_one, axis=0),
                jnp.sum(norm_one_grad, axis=0),
                jnp.sum(block_cotangent, axis=1),
            ]
        )
        feature_full = lax.dynamic_update_slice_in_dim(
            jnp.zeros((3, width), F32), feature_terms, w_index * feats, 1
        )
        fc_full = lax.dynamic_update_slice_in_dim(jnp.zeros((narrow * hid,), F32), fc_terms, n_index * hid, 0)
        token_sum, feature_sum, fc_sum = lax.psum((wide_terms, feature_full, fc_full), ("dp", "wide", "narrow"))
        gain_one, shift_one, proj_bias = lax.dynamic_slice_in_dim(feature_sum, w_index * feats, feats, 1)
        grad_b_fc = lax.dynamic_slice_in_dim(fc_sum, n_index * hid, hid, 0)
    grad_b_qv = lax.dynamic_slice_in_dim(token_sum[:2], n_index * part, part, 1)
    out_bias, gain_two, shift_two = lax.dynamic_slice_in_dim(token_sum[2:5], w_index * feats, feats, 1)
    return (
        output,
        grad_input,
        gain_one,
        shift_one,
        grad_w_qkv,
        grad_b_qv,
        grad_w_out,
        out_bias,
        gain_two,
        shift_two,
        grad_w_fc,
        grad_b_fc,
        grad_w_proj,
        proj_bias,
    )


def solution(mesh):
    return jax.shard_map(
        local,
        mesh=mesh,
        in_specs=(
            P("wide", ("dp", "narrow")),
            P("wide", ("dp", "narrow")),
            P(("dp", "wide", "narrow"), None),
            P("wide"),
            P("wide"),
            P("wide", None, "narrow"),
            P(None, "narrow"),
            P("wide", "narrow"),
            P("wide"),
            P("wide"),
            P("wide"),
            P("wide", "narrow"),
            P("narrow"),
            P("wide", "narrow"),
            P("wide"),
        ),
        out_specs=(
            P("wide", ("dp", "narrow")),
            P("wide", ("dp", "narrow")),
            P("wide"),
            P("wide"),
            P("wide", None, "narrow"),
            P(None, "narrow"),
            P("wide", "narrow"),
            P("wide"),
            P("wide"),
            P("wide"),
            P("wide", "narrow"),
            P("narrow"),
            P("wide", "narrow"),
            P("wide"),
        ),
        check_vma=False,
    )
```
